32 devices in a mesh: parts: 2 (over x), space: 16 (over z, y, core).
Axes of the slice: x: 2, y: 2, z: 4, core: 2. Of those that a mesh axis runs over, the one named last changes fastest.
Arguments:
- state: float32 [66, 64, 8, 256], P('parts', 'space'), parts along dimension 0, may hold values from 0.25 to 6.5
- adjoint: float32 [64, 64, 8, 256], P('parts', 'space'), parts along dimension 0, may hold values from -6 to 6
- control: float32 [64, 64, 8, 256], P('parts', 'space'), parts along dimension 0, may hold values from -6 to 6
- target: float32 [64, 128], P('parts'), parts along dimension 0, may hold values from 1 to 3
- mask: int32 [64, 16], P('space', 'parts'), parts along dimension 1, may hold values 0 or 1
- regions: int32 [64, 16, 256], P('space', 'parts'), parts along dimension 1, may hold values from 0 to 127, as said below
Outputs:
- state_spectrum: float32 [2, 64, 64, 8, 256], P(None, 'parts', 'space'), parts along dimension 1
- adjoint_spectrum: float32 [2, 64, 64, 8, 256], P(None, 'parts', 'space'), parts along dimension 1
- gradient_residual: float32 [64, 64, 8, 256], P('parts', 'space'), parts along dimension 0
The draws below stay inside these ranges and needn't reach their ends.
There are 2 independent parts, one for each index of `parts`. The reference program is written for one: setup_inputs(seed, part) draws one part's arguments, and reference() takes and returns one part's arrays. A program takes and returns all parts, laid end to end along the dimension named above; each array names one. Nothing has to cross between parts.
Inputs may be any that keep to these rules, and one draw needn't show every extreme that they name: `regions`: every region number from 0 to 127 labels at least one cell.
All inputs are finite; a program needn't handle non-finite values. No bound on the sum of `mask` on one device may be relied on, other than what follows from the above.
Results may differ from the reference program's by a relative error of at most 0.000098.
Values sent between devices are 32-bit elements; how exact they have to be, the bound alone decides.
A program may use at most 64 MiB of HBM per device.

```python
import jax
import jax.numpy as jnp

ZW = 8
NX = 256
NT = 32
REGIONS = 128
NY = 64


def draw_state(key, part):
    first = jax.random.fold_in(key, 0)
    row_index = jnp.arange(NY, dtype=jnp.float32)
    ramp = (1.0 + 2.0 * row_index / max(NY - 1, 1))[None, :, None, None]
    rough = jax.random.uniform(first, (NT + 1, NY, ZW, NX), jnp.float32, 0.5, 1.5)
    return ramp * rough


def draw_regions(key, part):
    tile_rows = 8
    tile_columns = REGIONS // tile_rows
    key_cuts = jax.random.fold_in(key, 11)
    key_shift = jax.random.fold_in(key, 12)
    key_label = jax.random.fold_in(key, 13)
    shuffled = jax.random.permutation(key_cuts, NY - 1).astype(jnp.int32)
    cut_points = jnp.sort(shuffled[:tile_rows - 1] + 1)
    row_index = jnp.arange(NY, dtype=jnp.int32)
    row_block = jnp.sum((cut_points[None, :] <= row_index[:, None]).astype(jnp.int32), axis=1)
    shifts = jax.random.randint(key_shift, (tile_rows,), 0, NX, dtype=jnp.int32)
    column_index = jnp.arange(NX, dtype=jnp.int32)
    shifted = column_index[None, :] + shifts[:, None]
    column_block = shifted * tile_columns // NX % tile_columns
    labels = jax.random.permutation(key_label, REGIONS).astype(jnp.int32)
    tile_index = row_block[:, None] * tile_columns + column_block[row_block]
    labelled = labels[tile_index]
    return jnp.broadcast_to(labelled[:, None, :], (NY, ZW, NX)).astype(jnp.int32)


def place_ends(entries, key, low, top_value):
    longest = entries.shape.index(max(entries.shape))
    spots = []
    for shift in (0, 1):
        where = [jax.random.randint(jax.random.fold_in(key, axis), (), 0, length) for axis, length in enumerate(entries.shape)]
        where[longest] = (where[longest] + shift) % entries.shape[longest]
        spots.append(tuple(where))
    return entries.at[spots[0]].set(low).at[spots[1]].set(top_value)


def block_scale(stream_key, shape, cuts, least, largest):
    loudness = 1.0
    for position, blocks in cuts:
        draws = jax.random.uniform(jax.random.fold_in(jax.random.fold_in(stream_key, 6), position), (blocks,), jnp.float32, least / len(cuts), largest / len(cuts))
        loudness = loudness * jnp.repeat(jnp.exp(draws), shape[position] // blocks).reshape((-1,) + (1,) * (len(shape) - 1 - position))
    return loudness


def noise(rng, dims, spread, bound, pieces=(), kind=jnp.bfloat16):
    factor_of = block_scale(rng, dims, pieces, -0.22, 0.18) if pieces else 1.0
    array = jax.random.normal(rng, dims, jnp.float32) * spread * factor_of
    return jnp.minimum(jnp.maximum(array, -bound), bound).astype(kind)


def setup_inputs(seed: int = 0, part: int = 0) -> dict:
    key_of = jax.random.split(jax.random.key(seed), 7)
    part_keys = jax.random.split(jax.random.fold_in(key_of[6], part), 7)
    state = draw_state(jax.random.fold_in(jax.random.fold_in(key_of[6], part), 71), part)
    adjoint = noise(part_keys[1], (NT, NY, ZW, NX), 1.0, 6.0, ((1, 16),), jnp.float32)
    control = noise(part_keys[2], (NT, NY, ZW, NX), 1.0, 6.0, ((1, 16),), jnp.float32)
    target = jnp.clip(jax.random.uniform(part_keys[3], (NT, REGIONS), jnp.float32, 1.0, 3.0), 1.0, 3.0)
    mask = place_ends((jax.random.randint(part_keys[4], (NY, ZW), 0, 2) < 1).astype(jnp.int32), jax.random.fold_in(part_keys[4], 1), 0, 1)
    regions = draw_regions(jax.random.fold_in(jax.random.fold_in(key_of[6], part), 71), part)
    return dict(state=state, adjoint=adjoint, control=control, target=target, mask=mask, regions=regions)


time_step = 0.15
penalty = 0.5


def laplace(values):
    across = jnp.roll(values, 1, axis=1) + jnp.roll(values, -1, axis=1)
    padded = jnp.pad(values, ((0, 0), (0, 0), (1, 1), (1, 1)))
    across = across + padded[:, :, 2:, 1:-1] + padded[:, :, :-2, 1:-1]
    across = across + padded[:, :, 1:-1, 2:] + padded[:, :, 1:-1, :-2]
    return across - 6.0 * values


def spectrum(residual):
    transformed = jnp.fft.fft(residual, axis=0)
    return jnp.stack([jnp.real(transformed), jnp.imag(transformed)], 0)


def reference(state, adjoint, control, target, mask, regions):
    support = mask.astype(jnp.float32)[None, :, :, None]
    earlier = state[:-1]
    advanced = state[1:]
    state_res = advanced - earlier - time_step * laplace(earlier) - time_step * support * control
    region_ids = regions.reshape(-1).astype(jnp.int32)
    unit_weight = jnp.ones(region_ids.shape, jnp.float32)
    counts = jax.ops.segment_sum(unit_weight, region_ids, num_segments=REGIONS)
    region_sums = jax.ops.segment_sum(advanced.reshape(NT, -1).T, region_ids, num_segments=REGIONS)
    misfit = region_sums.T / counts - target
    source = misfit[:, region_ids].reshape(advanced.shape)
    following = jnp.concatenate([adjoint[1:], jnp.zeros_like(adjoint[:1])], 0)
    adjoint_res = adjoint - following - time_step * laplace(following) + source
    gradient_residual = penalty * control - support * adjoint
    return spectrum(state_res), spectrum(adjoint_res), gradient_residual
```

```python
import functools
import math

import jax
import jax.numpy as jnp
from jax import lax
from jax.experimental import pallas as pl
from jax.experimental.pallas import tpu as pltpu
from jax.sharding import PartitionSpec as P

time_step = 0.15
penalty = 0.5
MESH = pl.DeviceIdType.MESH
ANY = pl.BlockSpec(memory_space=pl.ANY)


def pieces(length, parts):
    step = -(-length // parts)
    return [(start, min(step, length - start)) for start in range(0, length, step)]


def exchange_kernel(
    count, state, adjoint, regions, state_halo, adjoint_halo, totals,
    held, labels, partial, paired, summed, gathered,
    load_sem, halo_send, halo_recv, pair_send, pair_recv, peer_send, peer_recv,
):
    steps, rows, planes, width = (
        state.shape[0] - 1, state.shape[1], state.shape[2], state.shape[3],
    )
    count_regions = totals.shape[1]
    half = count // 2
    me = lax.axis_index("space")
    group, core = me // 2, me % 2
    above, below = (me + 1) % count, (me + count - 1) % count
    partner = group * 2 + 1 - core
    peers = [((group + d) % half) * 2 + core for d in range(1, half)]

    blocks = width // 128
    loads = [pltpu.make_async_copy(regions, labels, load_sem.at[blocks])] + [
        pltpu.make_async_copy(
            state.at[pl.ds(1, steps), :, :, pl.ds(block * 128, 128)], held.at[block], load_sem.at[block]
        )
        for block in range(blocks)
    ]
    for load in loads:
        load.start()
    barrier = pltpu.get_barrier_semaphore()
    for other in [above, below] + peers:
        pl.semaphore_signal(barrier, inc=1, device_id={"space": other}, device_id_type=MESH)
    pl.semaphore_wait(barrier, 1 + half)

    copies = []
    for source, first, target, length in ((state, 0, state_halo, steps), (adjoint, 1, adjoint_halo, steps - 1)):
        for start, size in pieces(length, 2):
            for side, (row, other) in enumerate(((rows - 1, above), (0, below))):
                n = len(copies)
                copies.append(
                    pltpu.make_async_remote_copy(
                        src_ref=source.at[pl.ds(first + start, size), row],
                        dst_ref=target.at[side, pl.ds(start, size)],
                        send_sem=halo_send.at[n],
                        recv_sem=halo_recv.at[n],
                        device_id={"space": other},
                        device_id_type=MESH,
                    )
                )
    for copy in copies[:2]:
        copy.start()

    for load in loads:
        load.wait()
    flat = held.reshape(blocks, steps * rows * planes, 128)
    region_ids = lax.broadcasted_iota(jnp.int32, (count_regions, width), 0)

    def add_row(row, total):
        values = jnp.concatenate(
            [
                flat[block, pl.ds(row * planes + plane, steps, stride=rows * planes), :]
                for plane in range(planes)
                for block in range(blocks)
            ],
            axis=1,
        )
        high = values.astype(jnp.bfloat16)
        low = (values - high.astype(jnp.float32)).astype(jnp.bfloat16)
        ones = jnp.ones((16, planes * width), jnp.bfloat16)
        stacked = jnp.concatenate([high, low, ones], axis=0)
        onehot = jnp.concatenate(
            [
                (labels[row, pl.ds(plane, 1), :] == region_ids).astype(jnp.float32).astype(jnp.bfloat16)
                for plane in range(planes)
            ],
            axis=1,
        )
        return total + lax.dot_general(
            stacked, onehot, (((1,), (1,)), ((), ())), preferred_element_type=jnp.float32
        )

    total = lax.fori_loop(
        0, rows, add_row, jnp.zeros((2 * steps + 16, count_regions), jnp.float32)
    )
    partial[:steps] = total[:steps] + total[steps : 2 * steps]
    partial[steps:] = total[2 * steps : 2 * steps + 8]
    pair = pltpu.make_async_remote_copy(
        src_ref=partial, dst_ref=paired, send_sem=pair_send.at[0], recv_sem=pair_recv.at[0],
        device_id={"space": partner}, device_id_type=MESH,
    )
    pair.start()
    pair.wait()
    summed[...] = partial[...] + paired[...]
    sends = [
        pltpu.make_async_remote_copy(
            src_ref=summed, dst_ref=gathered.at[d], send_sem=peer_send.at[d], recv_sem=peer_recv.at[d],
            device_id={"space": peer}, device_id_type=MESH,
        )
        for d, peer in enumerate(peers)
    ]
    for send in sends:
        send.start()
    for copy in copies[2:]:
        copy.start()
    result = summed[...]
    for d, send in enumerate(sends):
        send.wait()
        result = result + gathered[d]
    totals[...] = result
    for copy in copies:
        copy.wait()


def exchange(count, state, adjoint, regions, count_regions):
    levels, rows, planes, width = state.shape
    steps = levels - 1
    padded = (steps + 8, count_regions)
    half = count // 2
    f32 = jnp.float32
    return pl.pallas_call(
        functools.partial(exchange_kernel, count),
        out_shape=(
            jax.ShapeDtypeStruct((2, steps, planes, width), f32),
            jax.ShapeDtypeStruct((2, steps - 1, planes, width), f32),
            jax.ShapeDtypeStruct(padded, f32),
        ),
        in_specs=[ANY] * 3,
        out_specs=(ANY, ANY, pl.BlockSpec(memory_space=pltpu.VMEM)),
        scratch_shapes=[
            pltpu.VMEM((width // 128, steps, rows, planes, 128), f32),
            pltpu.VMEM(regions.shape, jnp.int32),
            pltpu.VMEM(padded, f32),
            pltpu.VMEM(padded, f32),
            pltpu.VMEM(padded, f32),
            pltpu.VMEM((half - 1,) + padded, f32),
            pltpu.SemaphoreType.DMA((width // 128 + 1,)),
            pltpu.SemaphoreType.DMA((8,)),
            pltpu.SemaphoreType.DMA((8,)),
            pltpu.SemaphoreType.DMA((1,)),
            pltpu.SemaphoreType.DMA((1,)),
            pltpu.SemaphoreType.DMA((half - 1,)),
            pltpu.SemaphoreType.DMA((half - 1,)),
        ],
        compiler_params=pltpu.CompilerParams(collective_id=0, has_side_effects=True),
        name="exchange",
    )(state, adjoint, regions)


def times(value, scale):
    if scale == 1.0:
        return value
    if scale == -1.0:
        return -value
    return value * scale


def real_transform(values):
    n = len(values)
    if n == 1:
        return [values[0]], [None]
    if n % 2:
        real, imag = [], []
        for k in range(n // 2 + 1):
            angles = [2.0 * math.pi * (j * k % n) / n for j in range(n)]
            real.append(sum(v * math.cos(a) for v, a in zip(values, angles)))
            imag.append(None if k == 0 else sum(v * -math.sin(a) for v, a in zip(values, angles)))
        return real, imag
    even_re, even_im = real_transform(values[::2])
    odd_re, odd_im = real_transform(values[1::2])
    m = n // 2
    real, imag = [None] * (m + 1), [None] * (m + 1)
    for k in range(m // 2 + 1):
        a_re, a_im, b_re, b_im = even_re[k], even_im[k], odd_re[k], odd_im[k]
        if k == 0:
            real[0], real[m] = a_re + b_re, a_re - b_re
            continue
        if 2 * k == m:
            real[k], imag[k] = a_re, -b_re
            continue
        c, s = math.cos(2.0 * math.pi * k / n), math.sin(2.0 * math.pi * k / n)
        t_re, t_im = c * b_re + s * b_im, c * b_im - s * b_re
        real[k], imag[k] = a_re + t_re, a_im + t_im
        real[m - k], imag[m - k] = a_re - t_re, t_im - a_im
    return real, imag


def write_spectrum(buffer, row, lanes, real, imag, n):
    zero = jnp.zeros_like(real[0])
    for k in range(n):
        low = min(k, n - k)
        buffer[0, row, k, :, lanes] = real[low]
        value = imag[low]
        buffer[1, row, k, :, lanes] = zero if value is None else (value if k == low else -value)


def residual_kernel(
    state, adjoint, control, target, mask, regions, state_halo, adjoint_halo, totals,
    state_out, adjoint_out, gradient_out,
    held, multipliers, heat, labels, residual, table, misfits, state_buffer, adjoint_buffer, gradient,
    held_sem, mult_sem, heat_sem, label_sem, state_sem, adjoint_sem, gradient_sem,
):
    steps, rows, planes, width = control.shape
    lane_blocks = width // 128

    def state_row(y):
        source = state_halo.at[0] if y < 0 else state_halo.at[1] if y == rows else state.at[pl.ds(0, steps + 1), y]
        into = held.at[y + 1, pl.ds(0, steps)] if y < 0 or y == rows else held.at[y + 1]
        return pltpu.make_async_copy(source, into, held_sem.at[y + 1])

    def adjoint_row(y):
        source = adjoint_halo.at[0] if y < 0 else adjoint_halo.at[1] if y == rows else adjoint.at[pl.ds(0, steps), y]
        into = multipliers.at[y + 1, pl.ds(1, steps - 1)] if y < 0 or y == rows else multipliers.at[y + 1]
        return pltpu.make_async_copy(source, into, mult_sem.at[y + 1])

    control_rows = [
        pltpu.make_async_copy(control.at[pl.ds(0, steps), y], heat.at[y], heat_sem.at[y]) for y in range(rows)
    ]
    state_rows = {y: state_row(y) for y in range(-1, rows + 1)}
    adjoint_rows = {y: adjoint_row(y) for y in range(-1, rows + 1)}
    label_copy = pltpu.make_async_copy(regions, labels, label_sem.at[0])
    label_copy.start()
    state_rows[-1].start()
    adjoint_rows[-1].start()
    state_rows[0].start()
    adjoint_rows[0].start()
    for y in range(rows):
        state_rows[y + 1].start()
        adjoint_rows[y + 1].start()
        control_rows[y].start()

    misfits[...] = totals[:steps] / totals[steps : steps + 1] - target[...]
    real, imag = real_transform(
        [jnp.broadcast_to(misfits[pl.ds(j, 1), :], (8, misfits.shape[1])) for j in range(steps)]
    )
    for k in range(steps // 2 + 1):
        table[k] = real[k]
        if imag[k] is not None:
            table[steps // 2 + k] = imag[k]
    label_copy.wait()

    lane = lax.broadcasted_iota(jnp.int32, (planes, width), 1)
    plane = lax.broadcasted_iota(jnp.int32, (planes, width), 0)
    first_lane, last_lane = lane == 0, lane == width - 1
    first_plane, last_plane = plane == 0, plane == planes - 1

    def laplace(values, before, after):
        total = before + after
        total = total + jnp.where(first_lane, 0.0, pltpu.roll(values, 1, 1))
        total = total + jnp.where(last_lane, 0.0, pltpu.roll(values, width - 1, 1))
        total = total + jnp.where(first_plane, 0.0, pltpu.roll(values, 1, 0))
        total = total + jnp.where(last_plane, 0.0, pltpu.roll(values, planes - 1, 0))
        return total - 6.0 * values

    state_rows[-1].wait()
    adjoint_rows[-1].wait()
    state_rows[0].wait()
    adjoint_rows[0].wait()

    def one_row(y):
        support = mask[y]

        def state_step(j, carry):
            now = held[y + 1, j]
            lap = laplace(now, held[y, j], held[y + 2, j])
            force = heat[y, j]
            residual[j] = held[y + 1, j + 1] - now - time_step * lap - time_step * support * force
            gradient[y, j] = penalty * force - support * multipliers[y + 1, j]
            return carry

        lax.fori_loop(0, steps, state_step, 0, unroll=8)
        for block in range(lane_blocks):
            lanes = pl.ds(block * 128, 128)
            real, imag = real_transform([residual[j, :, lanes] for j in range(steps)])
            write_spectrum(state_buffer, y, lanes, real, imag, steps)

        def adjoint_step(j, carry):
            later = multipliers[y + 1, j + 1]
            lap = laplace(later, multipliers[y, j + 1], multipliers[y + 2, j + 1])
            residual[j] = multipliers[y + 1, j] - later - time_step * lap
            return carry

        lax.fori_loop(0, steps - 1, adjoint_step, 0, unroll=8)
        residual[steps - 1] = multipliers[y + 1, steps - 1]
        for block in range(lane_blocks):
            lanes = pl.ds(block * 128, 128)
            ids = labels[y, :, lanes]
            real, imag = real_transform([residual[j, :, lanes] for j in range(steps)])

            def looked_up(k):
                return jnp.take_along_axis(table[k], ids, axis=1, mode="promise_in_bounds")

            real = [v + looked_up(k) for k, v in enumerate(real)]
            imag = [None if v is None else v + looked_up(steps // 2 + k) for k, v in enumerate(imag)]
            write_spectrum(adjoint_buffer, y, lanes, real, imag, steps)

    def outputs(y):
        found = [pltpu.make_async_copy(gradient.at[y], gradient_out.at[pl.ds(0, steps), y], gradient_sem.at[y])]
        for part in range(2):
            found.append(
                pltpu.make_async_copy(
                    state_buffer.at[part, y], state_out.at[part, pl.ds(0, steps), y], state_sem.at[part, y]
                )
            )
            found.append(
                pltpu.make_async_copy(
                    adjoint_buffer.at[part, y], adjoint_out.at[part, pl.ds(0, steps), y], adjoint_sem.at[part, y]
                )
            )
        return found

    def row_body(y, carry):
        for when in range(rows):
            @pl.when(y == when)
            def _():
                state_rows[when + 1].wait()
                adjoint_rows[when + 1].wait()
                control_rows[when].wait()

        one_row(y)
        for copy in outputs(y):
            copy.start()
        return carry

    lax.fori_loop(0, rows, row_body, 0)
    for y in range(rows):
        for copy in outputs(y):
            copy.wait()


def residuals(state, adjoint, control, target, support, regions, state_halo, adjoint_halo, totals):
    steps, rows, planes, width = control.shape
    f32 = jnp.float32
    vmem = pl.BlockSpec(memory_space=pltpu.VMEM)
    spectrum_shape = jax.ShapeDtypeStruct((2,) + control.shape, f32)
    dma = pltpu.SemaphoreType.DMA
    return pl.pallas_call(
        residual_kernel,
        out_shape=(spectrum_shape, spectrum_shape, jax.ShapeDtypeStruct(control.shape, f32)),
        in_specs=[ANY, ANY, ANY, vmem, vmem, ANY, ANY, ANY, vmem],
        out_specs=(ANY, ANY, ANY),
        scratch_shapes=[
            pltpu.VMEM((rows + 2, steps + 1, planes, width), f32),
            pltpu.VMEM((rows + 2, steps, planes, width), f32),
            pltpu.VMEM((rows, steps, planes, width), f32),
            pltpu.VMEM(regions.shape, jnp.int32),
            pltpu.VMEM((steps, planes, width), f32),
            pltpu.VMEM((steps, 8, target.shape[1]), f32),
            pltpu.VMEM(target.shape, f32),
            pltpu.VMEM((2, rows, steps, planes, width), f32),
            pltpu.VMEM((2, rows, steps, planes, width), f32),
            pltpu.VMEM((rows, steps, planes, width), f32),
            dma((rows + 2,)),
            dma((rows + 2,)),
            dma((rows,)),
            dma((1,)),
            dma((2, rows)),
            dma((2, rows)),
            dma((rows,)),
        ],
        name="residuals",
    )(state, adjoint, control, target, support, regions, state_halo, adjoint_halo, totals)


def on_device(count, state, adjoint, control, target, mask, regions):
    width = control.shape[3]
    support = jnp.broadcast_to(mask.astype(jnp.float32)[:, :, None], mask.shape + (width,))
    state_halo, adjoint_halo, totals = exchange(count, state, adjoint, regions, target.shape[1])
    return residuals(
        state, adjoint, control, target, support, regions, state_halo, adjoint_halo, totals
    )


def solution(mesh):
    return jax.shard_map(
        functools.partial(on_device, mesh.shape["space"]),
        mesh=mesh,
        in_specs=(
            P("parts", "space", None, None),
            P("parts", "space", None, None),
            P("parts", "space", None, None),
            P("parts", None),
            P("space", "parts"),
            P("space", "parts", None),
        ),
        out_specs=(
            P(None, "parts", "space", None, None),
            P(None, "parts", "space", None, None),
            P("parts", "space", None, None),
        ),
        check_vma=False,
    )
```

```python
import functools
import math

import jax
import jax.numpy as jnp
from jax import lax
from jax.experimental import pallas as pl
from jax.experimental.pallas import tpu as pltpu
from jax.sharding import PartitionSpec as P

time_step = 0.15
penalty = 0.5
MESH = pl.DeviceIdType.MESH
ANY = pl.BlockSpec(memory_space=pl.ANY)


def real_transform(values):
    n = len(values)
    if n == 1:
        return [values[0]], [None]
    if n % 2:
        real, imag = [], []
        for k in range(n // 2 + 1):
            angles = [2.0 * math.pi * (j * k % n) / n for j in range(n)]
            real.append(sum(v * math.cos(a) for v, a in zip(values, angles)))
            imag.append(None if k == 0 else sum(v * -math.sin(a) for v, a in zip(values, angles)))
        return real, imag
    even_re, even_im = real_transform(values[::2])
    odd_re, odd_im = real_transform(values[1::2])
    m = n // 2
    real, imag = [None] * (m + 1), [None] * (m + 1)
    for k in range(m // 2 + 1):
        a_re, a_im, b_re, b_im = even_re[k], even_im[k], odd_re[k], odd_im[k]
        if k == 0:
            real[0], real[m] = a_re + b_re, a_re - b_re
            continue
        if 2 * k == m:
            real[k], imag[k] = a_re, -b_re
            continue
        c, s = math.cos(2.0 * math.pi * k / n), math.sin(2.0 * math.pi * k / n)
        t_re, t_im = c * b_re + s * b_im, c * b_im - s * b_re
        real[k], imag[k] = a_re + t_re, a_im + t_im
        real[m - k], imag[m - k] = a_re - t_re, t_im - a_im
    return real, imag


def write_spectrum(buffer, row, lanes, real, imag, n):
    zero = jnp.zeros_like(real[0])
    for k in range(n):
        low = min(k, n - k)
        buffer[0, row, k, :, lanes] = real[low]
        value = imag[low]
        buffer[1, row, k, :, lanes] = zero if value is None else (value if k == low else -value)


def pack(real, imag):
    return real + [value for value in imag if value is not None]


def solve_kernel(
    count, state, adjoint, control, regions, target, mask,
    state_buffer, packed, gradient, table,
    sampled, held, multipliers, heat, labels, residual, partial, paired, summed, gathered,
    label_sem, sample_sem, held_sem, mult_sem, heat_sem,
    halo_send, halo_recv, pair_send, pair_recv, peer_send, peer_recv,
):
    steps, rows, planes, width = control.shape
    count_regions = target.shape[1]
    blocks = width // 128
    half = count // 2
    me = lax.axis_index("space")
    group, core = me // 2, me % 2
    above, below = (me + 1) % count, (me + count - 1) % count
    partner = group * 2 + 1 - core
    peers = [((group + d) % half) * 2 + core for d in range(1, half)]

    barrier = pltpu.get_barrier_semaphore()
    for other in [above, below] + peers:
        pl.semaphore_signal(barrier, inc=1, device_id={"space": other}, device_id_type=MESH)

    sums_loads = [pltpu.make_async_copy(regions, labels, label_sem.at[0])] + [
        pltpu.make_async_copy(
            state.at[pl.ds(1, steps), :, :, pl.ds(block * 128, 128)],
            sampled.at[block], sample_sem.at[block],
        )
        for block in range(blocks)
    ]
    heat_loads, mult_loads, held_loads = [], [], []
    for y in range(rows):
        heat_loads.append(pltpu.make_async_copy(control.at[pl.ds(0, steps), y], heat.at[y], heat_sem.at[y]))
        mult_loads.append(
            pltpu.make_async_copy(adjoint.at[pl.ds(0, steps), y], multipliers.at[y + 1], mult_sem.at[y])
        )
        held_loads.append(
            pltpu.make_async_copy(state.at[pl.ds(0, steps + 1), y], held.at[y + 1], held_sem.at[y])
        )
    for load in sums_loads + heat_loads + mult_loads + held_loads:
        load.start()

    copies = []
    for source, first, target_rows, shift, length in (
        (state, 0, held, 0, steps), (adjoint, 1, multipliers, 1, steps - 1),
    ):
        for block in range(blocks):
            lanes = pl.ds(block * 128, 128)
            for row, into, other in ((rows - 1, 0, above), (0, rows + 1, below)):
                n = len(copies)
                copies.append(
                    pltpu.make_async_remote_copy(
                        src_ref=source.at[pl.ds(first, length), row, :, lanes],
                        dst_ref=target_rows.at[into, pl.ds(shift, length), :, lanes],
                        send_sem=halo_send.at[n],
                        recv_sem=halo_recv.at[n],
                        device_id={"space": other},
                        device_id_type=MESH,
                    )
                )

    flat = sampled.reshape(blocks, steps * rows * planes, 128)
    region_ids = lax.broadcasted_iota(jnp.int32, (count_regions, width), 0)

    def add_row(row, total):
        values = jnp.concatenate(
            [
                flat[block, pl.ds(row * planes + plane, steps, stride=rows * planes), :]
                for plane in range(planes)
                for block in range(blocks)
            ],
            axis=1,
        )
        high = values.astype(jnp.bfloat16)
        low = (values - high.astype(jnp.float32)).astype(jnp.bfloat16)
        ones = jnp.ones((16, planes * width), jnp.bfloat16)
        stacked = jnp.concatenate([high, low, ones], axis=0)
        onehot = jnp.concatenate(
            [
                (labels[row, pl.ds(plane, 1), :] == region_ids).astype(jnp.float32).astype(jnp.bfloat16)
                for plane in range(planes)
            ],
            axis=1,
        )
        return total + lax.dot_general(
            stacked, onehot, (((1,), (1,)), ((), ())), preferred_element_type=jnp.float32
        )

    for load in sums_loads:
        load.wait()
    early = rows // 2
    total = jnp.zeros((2 * steps + 16, count_regions), jnp.float32)
    total = lax.fori_loop(0, early, add_row, total)
    pl.semaphore_wait(barrier, 1 + half)
    for copy in copies[:2]:
        copy.start()
    total = lax.fori_loop(early, rows, add_row, total)
    partial[:steps] = total[:steps] + total[steps : 2 * steps]
    partial[steps:] = total[2 * steps : 2 * steps + 8]
    pair = pltpu.make_async_remote_copy(
        src_ref=partial, dst_ref=paired, send_sem=pair_send.at[0], recv_sem=pair_recv.at[0],
        device_id={"space": partner}, device_id_type=MESH,
    )
    pair.start()

    lane = lax.broadcasted_iota(jnp.int32, (planes, width), 1)
    plane_ids = lax.broadcasted_iota(jnp.int32, (planes, width), 0)
    first_lane, last_lane = lane == 0, lane == width - 1
    first_plane, last_plane = plane_ids == 0, plane_ids == planes - 1

    def support_of(y):
        support = jnp.zeros((planes, width), jnp.float32)
        for plane in range(planes):
            support = jnp.where(plane_ids == plane, mask[y, plane].astype(jnp.float32), support)
        return support

    for load in heat_loads + mult_loads:
        load.wait()

    def gradient_row(y, carry):
        support = support_of(y)

        def step(j, inner):
            gradient[y, j] = penalty * heat[y, j] - support * multipliers[y + 1, j]
            return inner

        return lax.fori_loop(0, steps, step, carry, unroll=8)

    lax.fori_loop(0, rows, gradient_row, 0)

    pair.wait()
    summed[...] = partial[...] + paired[...]
    sends = [
        pltpu.make_async_remote_copy(
            src_ref=summed, dst_ref=gathered.at[d], send_sem=peer_send.at[d], recv_sem=peer_recv.at[d],
            device_id={"space": peer}, device_id_type=MESH,
        )
        for d, peer in enumerate(peers)
    ]
    for send in sends:
        send.start()
    for copy in copies[2:]:
        copy.start()

    def laplace(values, beside):
        total = beside + jnp.where(first_lane, 0.0, pltpu.roll(values, 1, 1))
        total = total + jnp.where(last_lane, 0.0, pltpu.roll(values, width - 1, 1))
        total = total + jnp.where(first_plane, 0.0, pltpu.roll(values, 1, 0))
        total = total + jnp.where(last_plane, 0.0, pltpu.roll(values, planes - 1, 0))
        return total - 6.0 * values

    def adjoint_transform(y, beside):
        def step(j, carry):
            later = multipliers[y + 1, j + 1]
            residual[j] = multipliers[y + 1, j] - later - time_step * laplace(later, beside(j + 1))
            return carry

        lax.fori_loop(0, steps - 1, step, 0, unroll=8)
        residual[steps - 1] = multipliers[y + 1, steps - 1]
        for block in range(blocks):
            lanes = pl.ds(block * 128, 128)
            values = real_transform([residual[j, :, lanes] for j in range(steps)])
            for k, value in enumerate(pack(*values)):
                packed[y, k, :, lanes] = value

    def adjoint_inner(y, carry):
        adjoint_transform(y, lambda j: multipliers[y, j] + multipliers[y + 2, j])
        return carry

    def adjoint_edge(side, carry):
        adjoint_transform(side * (rows - 1), lambda j: multipliers[2 + side * (rows - 3), j])
        return carry

    def state_row(y, carry):
        support = support_of(y)

        def step(j, inner):
            now = held[y + 1, j]
            lap = laplace(now, held[y, j] + held[y + 2, j])
            residual[j] = held[y + 1, j + 1] - now - time_step * lap - time_step * support * heat[y, j]
            return inner

        lax.fori_loop(0, steps, step, 0, unroll=8)
        for block in range(blocks):
            lanes = pl.ds(block * 128, 128)
            real, imag = real_transform([residual[j, :, lanes] for j in range(steps)])
            write_spectrum(state_buffer, y, lanes, real, imag, steps)
        return carry

    lax.fori_loop(1, rows - 1, adjoint_inner, 0)
    lax.fori_loop(0, 2, adjoint_edge, 0)
    for load in held_loads:
        load.wait()
    lax.fori_loop(1, rows - 1, state_row, 0)
    for copy in copies[: 2 * blocks]:
        copy.wait()
    lax.fori_loop(0, 2, lambda side, carry: state_row(side * (rows - 1), carry), 0)

    result = summed[...]
    for d, send in enumerate(sends):
        send.wait()
        result = result + gathered[d]
    misfit = result[:steps] / result[steps : steps + 1] - target[...]
    values = real_transform(
        [jnp.broadcast_to(misfit[j : j + 1], (8, count_regions)) for j in range(steps)]
    )
    for k, value in enumerate(pack(*values)):
        table[k] = value

    for block in range(blocks):
        lanes = pl.ds(block * 128, 128)
        for side in range(2):
            copies[2 * (blocks + block) + side].wait()

        def add_halo(side, carry):
            y, outer = side * (rows - 1), side * (rows + 1)
            values = [-time_step * multipliers[outer, j + 1, :, lanes] for j in range(steps - 1)]
            values.append(jnp.zeros_like(values[0]))
            for k, value in enumerate(pack(*real_transform(values))):
                packed[y, k, :, lanes] += value
            return carry

        lax.fori_loop(0, 2, add_halo, 0)


def solve(count, state, adjoint, control, regions, target, mask):
    steps, rows, planes, width = control.shape
    count_regions = target.shape[1]
    padded = (steps + 8, count_regions)
    half, blocks = count // 2, width // 128
    f32, dma, vmem = jnp.float32, pltpu.SemaphoreType.DMA, pltpu.VMEM
    in_vmem = pl.BlockSpec(memory_space=pltpu.VMEM)
    return pl.pallas_call(
        functools.partial(solve_kernel, count),
        out_shape=(
            vmem((2, rows, steps, planes, width), f32),
            vmem((rows, steps, planes, width), f32),
            vmem((rows, steps, planes, width), f32),
            vmem((steps, 8, count_regions), f32),
        ),
        in_specs=[ANY] * 4 + [in_vmem, pl.BlockSpec(memory_space=pltpu.SMEM)],
        out_specs=(in_vmem,) * 4,
        scratch_shapes=[
            vmem((blocks, steps, rows, planes, 128), f32),
            vmem((rows + 2, steps + 1, planes, width), f32),
            vmem((rows + 2, steps, planes, width), f32),
            vmem((rows, steps, planes, width), f32),
            vmem(regions.shape, jnp.int32),
            vmem((steps, planes, width), f32),
            vmem(padded, f32),
            vmem(padded, f32),
            vmem(padded, f32),
            vmem((half - 1,) + padded, f32),
            dma((1,)),
            dma((blocks,)),
            dma((rows,)),
            dma((rows,)),
            dma((rows,)),
            dma((4 * blocks,)),
            dma((4 * blocks,)),
            dma((1,)),
            dma((1,)),
            dma((half - 1,)),
            dma((half - 1,)),
        ],
        compiler_params=pltpu.CompilerParams(
            collective_id=0, has_side_effects=True, vmem_limit_bytes=24 * 2**20
        ),
        name="solve",
    )(state, adjoint, control, regions, target, mask)


def finish_kernel(
    state_buffer, packed, gradient, table, labels,
    state_out, adjoint_out, gradient_out,
    adjoint_buffer, state_sem, adjoint_sem, gradient_sem,
):
    rows, steps, planes, width = gradient.shape
    early = []
    for y in range(rows):
        for part in range(2):
            early.append(
                pltpu.make_async_copy(
                    state_buffer.at[part, y], state_out.at[part, pl.ds(0, steps), y], state_sem.at[part, y]
                )
            )
        early.append(
            pltpu.make_async_copy(gradient.at[y], gradient_out.at[pl.ds(0, steps), y], gradient_sem.at[y])
        )
    for copy in early:
        copy.start()

    def outputs(y):
        return [
            pltpu.make_async_copy(
                adjoint_buffer.at[part, y], adjoint_out.at[part, pl.ds(0, steps), y], adjoint_sem.at[part, y]
            )
            for part in range(2)
        ]

    def row_body(y, carry):
        for block in range(width // 128):
            lanes = pl.ds(block * 128, 128)
            ids = labels[y, :, lanes]
            values = [
                packed[y, k, :, lanes] + jnp.take_along_axis(table[k], ids, axis=1, mode="promise_in_bounds")
                for k in range(steps)
            ]
            top = steps // 2 + 1
            imag = [None] + values[top:] + [None] * (2 * top - 1 - steps)
            write_spectrum(adjoint_buffer, y, lanes, values[:top], imag, steps)
        for copy in outputs(y):
            copy.start()
        return carry

    lax.fori_loop(0, rows, row_body, 0)
    for copy in early + [copy for y in range(rows) for copy in outputs(y)]:
        copy.wait()


def finish(control, state_buffer, packed, gradient, table, regions):
    steps, rows, planes, width = control.shape
    f32, dma = jnp.float32, pltpu.SemaphoreType.DMA
    in_vmem = pl.BlockSpec(memory_space=pltpu.VMEM)
    spectrum_shape = jax.ShapeDtypeStruct((2,) + control.shape, f32)
    return pl.pallas_call(
        finish_kernel,
        out_shape=(spectrum_shape, spectrum_shape, jax.ShapeDtypeStruct(control.shape, f32)),
        in_specs=[in_vmem] * 5,
        out_specs=(ANY,) * 3,
        scratch_shapes=[
            pltpu.VMEM((2, rows, steps, planes, width), f32),
            dma((2, rows)),
            dma((2, rows)),
            dma((rows,)),
        ],
        compiler_params=pltpu.CompilerParams(vmem_limit_bytes=16 * 2**20),
        name="finish",
    )(state_buffer, packed, gradient, table, regions)


def on_device(count, state, adjoint, control, target, mask, regions):
    found = solve(count, state, adjoint, control, regions, target, mask)
    return finish(control, *found, regions)


def solution(mesh):
    return jax.shard_map(
        functools.partial(on_device, mesh.shape["space"]),
        mesh=mesh,
        in_specs=(
            P("parts", "space", None, None),
            P("parts", "space", None, None),
            P("parts", "space", None, None),
            P("parts", None),
            P("space", "parts"),
            P("space", "parts", None),
        ),
        out_specs=(
            P(None, "parts", "space", None, None),
            P(None, "parts", "space", None, None),
            P("parts", "space", None, None),
        ),
        check_vma=False,
    )
```

```python
import functools
import math

import jax
import jax.numpy as jnp
from jax import lax
from jax.experimental import pallas as pl
from jax.experimental.pallas import tpu as pltpu
from jax.sharding import PartitionSpec as P

time_step = 0.15
penalty = 0.5
MESH = pl.DeviceIdType.MESH
HBM = pl.BlockSpec(memory_space=pltpu.HBM)


def real_transform(values):
    n = len(values)
    if n == 1:
        return [values[0]], [None]
    if n % 2:
        real, imag = [], []
        for k in range(n // 2 + 1):
            angles = [2.0 * math.pi * (j * k % n) / n for j in range(n)]
            real.append(sum(v * math.cos(a) for v, a in zip(values, angles)))
            imag.append(None if k == 0 else sum(v * -math.sin(a) for v, a in zip(values, angles)))
        return real, imag
    even_re, even_im = real_transform(values[::2])
    odd_re, odd_im = real_transform(values[1::2])
    m = n // 2
    real, imag = [None] * (m + 1), [None] * (m + 1)
    for k in range(m // 2 + 1):
        a_re, a_im, b_re, b_im = even_re[k], even_im[k], odd_re[k], odd_im[k]
        if k == 0:
            real[0], real[m] = a_re + b_re, a_re - b_re
            continue
        if 2 * k == m:
            real[k], imag[k] = a_re, -b_re
            continue
        c, s = math.cos(2.0 * math.pi * k / n), math.sin(2.0 * math.pi * k / n)
        t_re, t_im = c * b_re + s * b_im, c * b_im - s * b_re
        real[k], imag[k] = a_re + t_re, a_im + t_im
        real[m - k], imag[m - k] = a_re - t_re, t_im - a_im
    return real, imag


def write_spectrum(buffer, row, lanes, real, imag, n):
    zero = jnp.zeros_like(real[0])
    for k in range(n):
        low = min(k, n - k)
        buffer[0, row, k, :, lanes] = real[low]
        value = imag[low]
        buffer[1, row, k, :, lanes] = zero if value is None else (value if k == low else -value)


def pack(real, imag):
    return real + [value for value in imag if value is not None]


def solve_kernel(
    count, state, adjoint, control, regions, target, mask,
    state_buffer, packed, gradient, table, labels,
    sampled, held, multipliers, heat, wanted, allowed, residual, partial, paired, summed, gathered,
    small_sem, sample_sem, held_sem, mult_sem, heat_sem,
    halo_send, halo_recv, pair_send, pair_recv, peer_send, peer_recv,
):
    steps, rows, planes, width = control.shape
    count_regions = target.shape[1]
    blocks = width // 128
    half = count // 2
    me = lax.axis_index("space")
    group, core = me // 2, me % 2
    above, below = (me + 1) % count, (me + count - 1) % count
    partner = group * 2 + 1 - core
    peers = [((group + d) % half) * 2 + core for d in range(1, half)]

    barrier = pltpu.get_barrier_semaphore()
    for other in [above, below] + peers:
        pl.semaphore_signal(barrier, inc=1, device_id={"space": other}, device_id_type=MESH)

    sums_loads = [pltpu.make_async_copy(regions, labels, small_sem.at[0])] + [
        pltpu.make_async_copy(
            state.at[pl.ds(1, steps), :, :, pl.ds(block * 128, 128)],
            sampled.at[block], sample_sem.at[block],
        )
        for block in range(blocks)
    ]
    small_loads = [
        pltpu.make_async_copy(target, wanted, small_sem.at[1]),
        pltpu.make_async_copy(mask, allowed, small_sem.at[2]),
    ]
    heat_loads, mult_loads, held_loads = [], [], []
    for y in range(rows):
        heat_loads.append(pltpu.make_async_copy(control.at[pl.ds(0, steps), y], heat.at[y], heat_sem.at[y]))
        mult_loads.append(
            pltpu.make_async_copy(adjoint.at[pl.ds(0, steps), y], multipliers.at[y + 1], mult_sem.at[y])
        )
        held_loads.append(
            pltpu.make_async_copy(state.at[pl.ds(0, steps + 1), y], held.at[y + 1], held_sem.at[y])
        )
    for load in sums_loads + small_loads + heat_loads + mult_loads + held_loads:
        load.start()

    copies = []
    for source, first, target_rows, shift, length in (
        (state, 0, held, 0, steps), (adjoint, 1, multipliers, 1, steps - 1),
    ):
        for block in range(blocks):
            lanes = pl.ds(block * 128, 128)
            for row, into, other in ((rows - 1, 0, above), (0, rows + 1, below)):
                n = len(copies)
                copies.append(
                    pltpu.make_async_remote_copy(
                        src_ref=source.at[pl.ds(first, length), row, :, lanes],
                        dst_ref=target_rows.at[into, pl.ds(shift, length), :, lanes],
                        send_sem=halo_send.at[n],
                        recv_sem=halo_recv.at[n],
                        device_id={"space": other},
                        device_id_type=MESH,
                    )
                )

    flat = sampled.reshape(blocks, steps * rows * planes, 128)
    region_ids = lax.broadcasted_iota(jnp.int32, (count_regions, width), 0)

    def add_row(row, total):
        values = jnp.concatenate(
            [
                flat[block, pl.ds(row * planes + plane, steps, stride=rows * planes), :]
                for plane in range(planes)
                for block in range(blocks)
            ],
            axis=1,
        )
        high = values.astype(jnp.bfloat16)
        low = (values - high.astype(jnp.float32)).astype(jnp.bfloat16)
        ones = jnp.ones((16, planes * width), jnp.bfloat16)
        stacked = jnp.concatenate([high, low, ones], axis=0)
        onehot = jnp.concatenate(
            [
                (labels[row, pl.ds(plane, 1), :] == region_ids).astype(jnp.float32).astype(jnp.bfloat16)
                for plane in range(planes)
            ],
            axis=1,
        )
        return total + lax.dot_general(
            stacked, onehot, (((1,), (1,)), ((), ())), preferred_element_type=jnp.float32
        )

    for load in sums_loads:
        load.wait()
    early = rows // 2
    total = jnp.zeros((2 * steps + 16, count_regions), jnp.float32)
    total = lax.fori_loop(0, early, add_row, total)
    pl.semaphore_wait(barrier, 1 + half)
    for copy in copies[:2]:
        copy.start()
    total = lax.fori_loop(early, rows, add_row, total)
    partial[:steps] = total[:steps] + total[steps : 2 * steps]
    partial[steps:] = total[2 * steps : 2 * steps + 8]
    pair = pltpu.make_async_remote_copy(
        src_ref=partial, dst_ref=paired, send_sem=pair_send.at[0], recv_sem=pair_recv.at[0],
        device_id={"space": partner}, device_id_type=MESH,
    )
    pair.start()

    lane = lax.broadcasted_iota(jnp.int32, (planes, width), 1)
    plane_ids = lax.broadcasted_iota(jnp.int32, (planes, width), 0)
    first_lane, last_lane = lane == 0, lane == width - 1
    first_plane, last_plane = plane_ids == 0, plane_ids == planes - 1

    def support_of(y):
        support = jnp.zeros((planes, width), jnp.float32)
        for plane in range(planes):
            support = jnp.where(plane_ids == plane, allowed[y, plane].astype(jnp.float32), support)
        return support

    for load in small_loads + heat_loads + mult_loads:
        load.wait()

    def gradient_row(y, carry):
        support = support_of(y)

        def step(j, inner):
            gradient[y, j] = penalty * heat[y, j] - support * multipliers[y + 1, j]
            return inner

        return lax.fori_loop(0, steps, step, carry, unroll=8)

    lax.fori_loop(0, rows, gradient_row, 0)

    pair.wait()
    summed[...] = partial[...] + paired[...]
    sends = [
        pltpu.make_async_remote_copy(
            src_ref=summed, dst_ref=gathered.at[d], send_sem=peer_send.at[d], recv_sem=peer_recv.at[d],
            device_id={"space": peer}, device_id_type=MESH,
        )
        for d, peer in enumerate(peers)
    ]
    for send in sends:
        send.start()
    for copy in copies[2:]:
        copy.start()

    def laplace(values, beside):
        total = beside + jnp.where(first_lane, 0.0, pltpu.roll(values, 1, 1))
        total = total + jnp.where(last_lane, 0.0, pltpu.roll(values, width - 1, 1))
        total = total + jnp.where(first_plane, 0.0, pltpu.roll(values, 1, 0))
        total = total + jnp.where(last_plane, 0.0, pltpu.roll(values, planes - 1, 0))
        return total - 6.0 * values

    def adjoint_transform(y, beside):
        def step(j, carry):
            later = multipliers[y + 1, j + 1]
            residual[j] = multipliers[y + 1, j] - later - time_step * laplace(later, beside(j + 1))
            return carry

        lax.fori_loop(0, steps - 1, step, 0, unroll=8)
        residual[steps - 1] = multipliers[y + 1, steps - 1]
        for block in range(blocks):
            lanes = pl.ds(block * 128, 128)
            values = real_transform([residual[j, :, lanes] for j in range(steps)])
            for k, value in enumerate(pack(*values)):
                packed[y, k, :, lanes] = value

    def adjoint_inner(y, carry):
        adjoint_transform(y, lambda j: multipliers[y, j] + multipliers[y + 2, j])
        return carry

    def adjoint_edge(side, carry):
        adjoint_transform(side * (rows - 1), lambda j: multipliers[2 + side * (rows - 3), j])
        return carry

    def state_row(y, carry):
        support = support_of(y)

        def step(j, inner):
            now = held[y + 1, j]
            lap = laplace(now, held[y, j] + held[y + 2, j])
            residual[j] = held[y + 1, j + 1] - now - time_step * lap - time_step * support * heat[y, j]
            return inner

        lax.fori_loop(0, steps, step, 0, unroll=8)
        for block in range(blocks):
            lanes = pl.ds(block * 128, 128)
            real, imag = real_transform([residual[j, :, lanes] for j in range(steps)])
            write_spectrum(state_buffer, y, lanes, real, imag, steps)
        return carry

    lax.fori_loop(1, rows - 1, adjoint_inner, 0)
    lax.fori_loop(0, 2, adjoint_edge, 0)
    for load in held_loads:
        load.wait()
    lax.fori_loop(1, rows - 1, state_row, 0)
    for copy in copies[: 2 * blocks]:
        copy.wait()
    lax.fori_loop(0, 2, lambda side, carry: state_row(side * (rows - 1), carry), 0)

    result = summed[...]
    for d, send in enumerate(sends):
        send.wait()
        result = result + gathered[d]
    misfit = result[:steps] / result[steps : steps + 1] - wanted[...]
    values = real_transform(
        [jnp.broadcast_to(misfit[j : j + 1], (8, count_regions)) for j in range(steps)]
    )
    for k, value in enumerate(pack(*values)):
        table[k] = value

    for block in range(blocks):
        lanes = pl.ds(block * 128, 128)
        for side in range(2):
            copies[2 * (blocks + block) + side].wait()

        def add_halo(side, carry):
            y, outer = side * (rows - 1), side * (rows + 1)
            values = [-time_step * multipliers[outer, j + 1, :, lanes] for j in range(steps - 1)]
            values.append(jnp.zeros_like(values[0]))
            for k, value in enumerate(pack(*real_transform(values))):
                packed[y, k, :, lanes] += value
            return carry

        lax.fori_loop(0, 2, add_halo, 0)


def solve(count, state, adjoint, control, regions, target, mask):
    steps, rows, planes, width = control.shape
    count_regions = target.shape[1]
    padded = (steps + 8, count_regions)
    half, blocks = count // 2, width // 128
    f32, dma, vmem = jnp.float32, pltpu.SemaphoreType.DMA, pltpu.VMEM
    in_vmem = pl.BlockSpec(memory_space=pltpu.VMEM)
    return pl.pallas_call(
        functools.partial(solve_kernel, count),
        out_shape=(
            vmem((2, rows, steps, planes, width), f32),
            vmem((rows, steps, planes, width), f32),
            vmem((rows, steps, planes, width), f32),
            vmem((steps, 8, count_regions), f32),
            vmem(regions.shape, jnp.int32),
        ),
        in_specs=[HBM] * 6,
        out_specs=(in_vmem,) * 5,
        scratch_shapes=[
            vmem((blocks, steps, rows, planes, 128), f32),
            vmem((rows + 2, steps + 1, planes, width), f32),
            vmem((rows + 2, steps, planes, width), f32),
            vmem((rows, steps, planes, width), f32),
            vmem(target.shape, f32),
            pltpu.SMEM(mask.shape, jnp.int32),
            vmem((steps, planes, width), f32),
            vmem(padded, f32),
            vmem(padded, f32),
            vmem(padded, f32),
            vmem((half - 1,) + padded, f32),
            dma((3,)),
            dma((blocks,)),
            dma((rows,)),
            dma((rows,)),
            dma((rows,)),
            dma((4 * blocks,)),
            dma((4 * blocks,)),
            dma((1,)),
            dma((1,)),
            dma((half - 1,)),
            dma((half - 1,)),
        ],
        compiler_params=pltpu.CompilerParams(
            collective_id=0, has_side_effects=True, vmem_limit_bytes=24 * 2**20
        ),
        name="solve",
    )(state, adjoint, control, regions, target, mask)


def finish_kernel(
    state_buffer, packed, gradient, table, labels,
    state_out, adjoint_out, gradient_out,
    adjoint_buffer, state_sem, adjoint_sem, gradient_sem,
):
    rows, steps, planes, width = gradient.shape
    early = []
    for y in range(rows):
        for part in range(2):
            early.append(
                pltpu.make_async_copy(
                    state_buffer.at[part, y], state_out.at[part, pl.ds(0, steps), y], state_sem.at[part, y]
                )
            )
        early.append(
            pltpu.make_async_copy(gradient.at[y], gradient_out.at[pl.ds(0, steps), y], gradient_sem.at[y])
        )
    for copy in early:
        copy.start()

    def outputs(y):
        return [
            pltpu.make_async_copy(
                adjoint_buffer.at[part, y], adjoint_out.at[part, pl.ds(0, steps), y], adjoint_sem.at[part, y]
            )
            for part in range(2)
        ]

    def row_body(y, carry):
        for block in range(width // 128):
            lanes = pl.ds(block * 128, 128)
            ids = labels[y, :, lanes]
            values = [
                packed[y, k, :, lanes] + jnp.take_along_axis(table[k], ids, axis=1, mode="promise_in_bounds")
                for k in range(steps)
            ]
            top = steps // 2 + 1
            imag = [None] + values[top:] + [None] * (2 * top - 1 - steps)
            write_spectrum(adjoint_buffer, y, lanes, values[:top], imag, steps)
        for copy in outputs(y):
            copy.start()
        return carry

    lax.fori_loop(0, rows, row_body, 0)
    for copy in early + [copy for y in range(rows) for copy in outputs(y)]:
        copy.wait()


def finish(control, state_buffer, packed, gradient, table, labels):
    steps, rows, planes, width = control.shape
    f32, dma = jnp.float32, pltpu.SemaphoreType.DMA
    in_vmem = pl.BlockSpec(memory_space=pltpu.VMEM)
    spectrum_shape = jax.ShapeDtypeStruct((2,) + control.shape, f32)
    return pl.pallas_call(
        finish_kernel,
        out_shape=(spectrum_shape, spectrum_shape, jax.ShapeDtypeStruct(control.shape, f32)),
        in_specs=[in_vmem] * 5,
        out_specs=(HBM,) * 3,
        scratch_shapes=[
            pltpu.VMEM((2, rows, steps, planes, width), f32),
            dma((2, rows)),
            dma((2, rows)),
            dma((rows,)),
        ],
        compiler_params=pltpu.CompilerParams(vmem_limit_bytes=16 * 2**20),
        name="finish",
    )(state_buffer, packed, gradient, table, labels)


def on_device(count, *arrays):
    state, adjoint, control, target, mask, regions = (
        pltpu.with_memory_space_constraint(array, pltpu.HBM) for array in arrays
    )
    found = solve(count, state, adjoint, control, regions, target, mask)
    return finish(control, *found)


def solution(mesh):
    return jax.shard_map(
        functools.partial(on_device, mesh.shape["space"]),
        mesh=mesh,
        in_specs=(
            P("parts", "space", None, None),
            P("parts", "space", None, None),
            P("parts", "space", None, None),
            P("parts", None),
            P("space", "parts"),
            P("space", "parts", None),
        ),
        out_specs=(
            P(None, "parts", "space", None, None),
            P(None, "parts", "space", None, None),
            P("parts", "space", None, None),
        ),
        check_vma=False,
    )
```

```python
import functools
import math

import jax
import jax.numpy as jnp
from jax import lax
from jax.experimental import pallas as pl
from jax.experimental.pallas import tpu as pltpu
from jax.sharding import PartitionSpec as P

time_step = 0.15
penalty = 0.5
MESH = pl.DeviceIdType.MESH
HBM = pl.BlockSpec(memory_space=pltpu.HBM)


def real_transform(values):
    n = len(values)
    if n == 1:
        return [values[0]], [None]
    if n % 2:
        real, imag = [], []
        for k in range(n // 2 + 1):
            angles = [2.0 * math.pi * (j * k % n) / n for j in range(n)]
            real.append(sum(v * math.cos(a) for v, a in zip(values, angles)))
            imag.append(None if k == 0 else sum(v * -math.sin(a) for v, a in zip(values, angles)))
        return real, imag
    even_re, even_im = real_transform(values[::2])
    odd_re, odd_im = real_transform(values[1::2])
    m = n // 2
    real, imag = [None] * (m + 1), [None] * (m + 1)
    for k in range(m // 2 + 1):
        a_re, a_im, b_re, b_im = even_re[k], even_im[k], odd_re[k], odd_im[k]
        if k == 0:
            real[0], real[m] = a_re + b_re, a_re - b_re
            continue
        if 2 * k == m:
            real[k], imag[k] = a_re, -b_re
            continue
        c, s = math.cos(2.0 * math.pi * k / n), math.sin(2.0 * math.pi * k / n)
        t_re, t_im = c * b_re + s * b_im, c * b_im - s * b_re
        real[k], imag[k] = a_re + t_re, a_im + t_im
        real[m - k], imag[m - k] = a_re - t_re, t_im - a_im
    return real, imag


def write_spectrum(buffer, row, lanes, real, imag, n):
    zero = jnp.zeros_like(real[0])
    for k in range(n):
        low = min(k, n - k)
        buffer[0, row, k, :, lanes] = real[low]
        value = imag[low]
        buffer[1, row, k, :, lanes] = zero if value is None else (value if k == low else -value)


def pack(real, imag):
    return real + [value for value in imag if value is not None]


def solve_kernel(
    count, state, adjoint, control, regions, target, mask,
    state_buffer, packed, gradient, table, labels,
    sampled, held, multipliers, heat, wanted, allowed, residual, partial, paired, joined, crossed, summed, from_lower, from_upper, to_upper, to_lower,
    small_sem, sample_sem, held_sem, mult_sem, heat_sem,
    halo_send, halo_recv, pair_send, pair_recv, chain_send, chain_recv,
):
    steps, rows, planes, width = control.shape
    count_regions = target.shape[1]
    blocks = width // 128
    links = count // 4
    me = lax.axis_index("space")
    link, place = me // 4, me % 4
    above, below = (me + 1) % count, (me + count - 1) % count
    partner = (me // 2) * 2 + 1 - me % 2
    across = link * 4 + (place + 2) % 4
    upper, lower = (me + 4) % count, (me + count - 4) % count
    has_upper, has_lower = link < links - 1, link > 0

    barrier = pltpu.get_barrier_semaphore()

    def greet(other):
        pl.semaphore_signal(barrier, inc=1, device_id={"space": other}, device_id_type=MESH)

    for other in (above, below, across):
        greet(other)
    pl.when(has_upper)(lambda: greet(upper))
    pl.when(has_lower)(lambda: greet(lower))

    sums_loads = [pltpu.make_async_copy(regions, labels, small_sem.at[0])] + [
        pltpu.make_async_copy(
            state.at[pl.ds(1, steps), :, :, pl.ds(block * 128, 128)],
            sampled.at[block], sample_sem.at[block],
        )
        for block in range(blocks)
    ]
    small_loads = [
        pltpu.make_async_copy(target, wanted, small_sem.at[1]),
        pltpu.make_async_copy(mask, allowed, small_sem.at[2]),
    ]
    heat_loads, mult_loads, held_loads = [], [], []
    for y in range(rows):
        heat_loads.append(pltpu.make_async_copy(control.at[pl.ds(0, steps), y], heat.at[y], heat_sem.at[y]))
        mult_loads.append(
            pltpu.make_async_copy(adjoint.at[pl.ds(0, steps), y], multipliers.at[y + 1], mult_sem.at[y])
        )
        held_loads.append(
            pltpu.make_async_copy(state.at[pl.ds(0, steps + 1), y], held.at[y + 1], held_sem.at[y])
        )
    for load in sums_loads + small_loads + heat_loads + mult_loads + held_loads:
        load.start()

    copies = []
    for source, first, target_rows, shift, length in (
        (state, 0, held, 0, steps), (adjoint, 1, multipliers, 1, steps - 1),
    ):
        for block in range(blocks):
            lanes = pl.ds(block * 128, 128)
            for row, into, other in ((rows - 1, 0, above), (0, rows + 1, below)):
                n = len(copies)
                copies.append(
                    pltpu.make_async_remote_copy(
                        src_ref=source.at[pl.ds(first, length), row, :, lanes],
                        dst_ref=target_rows.at[into, pl.ds(shift, length), :, lanes],
                        send_sem=halo_send.at[n],
                        recv_sem=halo_recv.at[n],
                        device_id={"space": other},
                        device_id_type=MESH,
                    )
                )

    flat = sampled.reshape(blocks, steps * rows * planes, 128)
    region_ids = lax.broadcasted_iota(jnp.int32, (count_regions, width), 0)

    def add_row(row, total):
        values = jnp.concatenate(
            [
                flat[block, pl.ds(row * planes + plane, steps, stride=rows * planes), :]
                for plane in range(planes)
                for block in range(blocks)
            ],
            axis=1,
        )
        high = values.astype(jnp.bfloat16)
        low = (values - high.astype(jnp.float32)).astype(jnp.bfloat16)
        ones = jnp.ones((16, planes * width), jnp.bfloat16)
        stacked = jnp.concatenate([high, low, ones], axis=0)
        onehot = jnp.concatenate(
            [
                (labels[row, pl.ds(plane, 1), :] == region_ids).astype(jnp.float32).astype(jnp.bfloat16)
                for plane in range(planes)
            ],
            axis=1,
        )
        return total + lax.dot_general(
            stacked, onehot, (((1,), (1,)), ((), ())), preferred_element_type=jnp.float32
        )

    greeted = 3 + has_upper.astype(jnp.int32) + has_lower.astype(jnp.int32)
    pl.semaphore_wait(barrier, greeted)
    for copy in copies[:2]:
        copy.start()
    for load in sums_loads:
        load.wait()
    total = jnp.zeros((2 * steps + 16, count_regions), jnp.float32)
    total = lax.fori_loop(0, rows, add_row, total)
    partial[:steps] = total[:steps] + total[steps : 2 * steps]
    partial[steps:] = total[2 * steps : 2 * steps + 8]
    pair = pltpu.make_async_remote_copy(
        src_ref=partial, dst_ref=paired, send_sem=pair_send.at[0], recv_sem=pair_recv.at[0],
        device_id={"space": partner}, device_id_type=MESH,
    )
    pair.start()

    lane = lax.broadcasted_iota(jnp.int32, (planes, width), 1)
    plane_ids = lax.broadcasted_iota(jnp.int32, (planes, width), 0)
    first_lane, last_lane = lane == 0, lane == width - 1
    first_plane, last_plane = plane_ids == 0, plane_ids == planes - 1

    def support_of(y):
        support = jnp.zeros((planes, width), jnp.float32)
        for plane in range(planes):
            support = jnp.where(plane_ids == plane, allowed[y, plane].astype(jnp.float32), support)
        return support

    for load in small_loads + heat_loads + mult_loads:
        load.wait()

    def gradient_row(y, carry):
        support = support_of(y)

        def step(j, inner):
            gradient[y, j] = penalty * heat[y, j] - support * multipliers[y + 1, j]
            return inner

        return lax.fori_loop(0, steps, step, carry, unroll=8)

    lax.fori_loop(0, rows, gradient_row, 0)

    pair.wait()
    joined[...] = partial[...] + paired[...]
    cross = pltpu.make_async_remote_copy(
        src_ref=joined, dst_ref=crossed, send_sem=pair_send.at[1], recv_sem=pair_recv.at[1],
        device_id={"space": across}, device_id_type=MESH,
    )
    cross.start()
    for copy in copies[2:4]:
        copy.start()

    upward = pltpu.make_async_remote_copy(
        src_ref=to_upper, dst_ref=from_lower, send_sem=chain_send.at[0], recv_sem=chain_recv.at[0],
        device_id={"space": upper}, device_id_type=MESH,
    )
    downward = pltpu.make_async_remote_copy(
        src_ref=to_lower, dst_ref=from_upper, send_sem=chain_send.at[1], recv_sem=chain_recv.at[1],
        device_id={"space": lower}, device_id_type=MESH,
    )

    def pass_on(copy, arriving, leaving, has_source, has_target):
        pl.when(has_source)(copy.wait_recv)

        @pl.when(jnp.logical_not(has_source))
        def _():
            arriving[...] = jnp.zeros_like(arriving)

        @pl.when(has_target)
        def _():
            leaving[...] = arriving[...] + summed[...]
            copy.start()

    def pass_up():
        pass_on(upward, from_lower, to_upper, has_lower, has_upper)

    def pass_down():
        pass_on(downward, from_upper, to_lower, has_upper, has_lower)

    near_bottom = link < links // 2

    def laplace(values, beside):
        total = beside + jnp.where(first_lane, 0.0, pltpu.roll(values, 1, 1))
        total = total + jnp.where(last_lane, 0.0, pltpu.roll(values, width - 1, 1))
        total = total + jnp.where(first_plane, 0.0, pltpu.roll(values, 1, 0))
        total = total + jnp.where(last_plane, 0.0, pltpu.roll(values, planes - 1, 0))
        return total - 6.0 * values

    def adjoint_transform(y, beside):
        def step(j, carry):
            later = multipliers[y + 1, j + 1]
            residual[j] = multipliers[y + 1, j] - later - time_step * laplace(later, beside(j + 1))
            return carry

        lax.fori_loop(0, steps - 1, step, 0, unroll=8)
        residual[steps - 1] = multipliers[y + 1, steps - 1]
        for block in range(blocks):
            lanes = pl.ds(block * 128, 128)
            values = real_transform([residual[j, :, lanes] for j in range(steps)])
            for k, value in enumerate(pack(*values)):
                packed[y, k, :, lanes] = value

    def adjoint_inner(y, carry):
        adjoint_transform(y, lambda j: multipliers[y, j] + multipliers[y + 2, j])
        return carry

    def adjoint_edge(side, carry):
        adjoint_transform(side * (rows - 1), lambda j: multipliers[2 + side * (rows - 3), j])
        return carry

    def state_row(y, carry):
        support = support_of(y)

        def step(j, inner):
            now = held[y + 1, j]
            lap = laplace(now, held[y, j] + held[y + 2, j])
            residual[j] = held[y + 1, j + 1] - now - time_step * lap - time_step * support * heat[y, j]
            return inner

        lax.fori_loop(0, steps, step, 0, unroll=8)
        for block in range(blocks):
            lanes = pl.ds(block * 128, 128)
            real, imag = real_transform([residual[j, :, lanes] for j in range(steps)])
            write_spectrum(state_buffer, y, lanes, real, imag, steps)
        return carry

    lax.fori_loop(1, rows - 1, adjoint_inner, 0)
    cross.wait()
    summed[...] = joined[...] + crossed[...]
    pl.when(near_bottom)(pass_up)
    pl.when(jnp.logical_not(near_bottom))(pass_down)
    for copy in copies[4:]:
        copy.start()
    lax.fori_loop(0, 2, adjoint_edge, 0)
    pl.when(near_bottom)(pass_down)
    pl.when(jnp.logical_not(near_bottom))(pass_up)
    for load in held_loads:
        load.wait()
    lax.fori_loop(1, rows - 1, state_row, 0)
    for copy in copies[: 2 * blocks]:
        copy.wait()
    lax.fori_loop(0, 2, lambda side, carry: state_row(side * (rows - 1), carry), 0)

    result = summed[...] + from_lower[...] + from_upper[...]
    pl.when(has_upper)(upward.wait_send)
    pl.when(has_lower)(downward.wait_send)
    misfit = result[:steps] / result[steps : steps + 1] - wanted[...]
    values = real_transform(
        [jnp.broadcast_to(misfit[j : j + 1], (8, count_regions)) for j in range(steps)]
    )
    for k, value in enumerate(pack(*values)):
        table[k] = value

    for block in range(blocks):
        lanes = pl.ds(block * 128, 128)
        for side in range(2):
            copies[2 * (blocks + block) + side].wait()

        def add_halo(side, carry):
            y, outer = side * (rows - 1), side * (rows + 1)
            values = [-time_step * multipliers[outer, j + 1, :, lanes] for j in range(steps - 1)]
            values.append(jnp.zeros_like(values[0]))
            for k, value in enumerate(pack(*real_transform(values))):
                packed[y, k, :, lanes] += value
            return carry

        lax.fori_loop(0, 2, add_halo, 0)


def solve(count, state, adjoint, control, regions, target, mask):
    steps, rows, planes, width = control.shape
    count_regions = target.shape[1]
    padded = (steps + 8, count_regions)
    blocks = width // 128
    f32, dma, vmem = jnp.float32, pltpu.SemaphoreType.DMA, pltpu.VMEM
    in_vmem = pl.BlockSpec(memory_space=pltpu.VMEM)
    return pl.pallas_call(
        functools.partial(solve_kernel, count),
        out_shape=(
            vmem((2, rows, steps, planes, width), f32),
            vmem((rows, steps, planes, width), f32),
            vmem((rows, steps, planes, width), f32),
            vmem((steps, 8, count_regions), f32),
            vmem(regions.shape, jnp.int32),
        ),
        in_specs=[HBM] * 6,
        out_specs=(in_vmem,) * 5,
        scratch_shapes=[
            vmem((blocks, steps, rows, planes, 128), f32),
            vmem((rows + 2, steps + 1, planes, width), f32),
            vmem((rows + 2, steps, planes, width), f32),
            vmem((rows, steps, planes, width), f32),
            vmem(target.shape, f32),
            pltpu.SMEM(mask.shape, jnp.int32),
            vmem((steps, planes, width), f32),
        ]
        + [vmem(padded, f32)] * 9
        + [
            dma((3,)),
            dma((blocks,)),
            dma((rows,)),
            dma((rows,)),
            dma((rows,)),
            dma((4 * blocks,)),
            dma((4 * blocks,)),
            dma((2,)),
            dma((2,)),
            dma((2,)),
            dma((2,)),
        ],
        compiler_params=pltpu.CompilerParams(
            collective_id=0, has_side_effects=True, vmem_limit_bytes=24 * 2**20
        ),
        name="solve",
    )(state, adjoint, control, regions, target, mask)


def finish_kernel(
    state_buffer, packed, gradient, table, labels,
    state_out, adjoint_out, gradient_out,
    adjoint_buffer, state_sem, adjoint_sem, gradient_sem,
):
    rows, steps, planes, width = gradient.shape
    early = []
    for y in range(rows):
        for part in range(2):
            early.append(
                pltpu.make_async_copy(
                    state_buffer.at[part, y], state_out.at[part, pl.ds(0, steps), y], state_sem.at[part, y]
                )
            )
        early.append(
            pltpu.make_async_copy(gradient.at[y], gradient_out.at[pl.ds(0, steps), y], gradient_sem.at[y])
        )
    for copy in early:
        copy.start()

    def outputs(y):
        return [
            pltpu.make_async_copy(
                adjoint_buffer.at[part, y], adjoint_out.at[part, pl.ds(0, steps), y], adjoint_sem.at[part, y]
            )
            for part in range(2)
        ]

    def row_body(y, carry):
        for block in range(width // 128):
            lanes = pl.ds(block * 128, 128)
            ids = labels[y, :, lanes]
            values = [
                packed[y, k, :, lanes] + jnp.take_along_axis(table[k], ids, axis=1, mode="promise_in_bounds")
                for k in range(steps)
            ]
            top = steps // 2 + 1
            imag = [None] + values[top:] + [None] * (2 * top - 1 - steps)
            write_spectrum(adjoint_buffer, y, lanes, values[:top], imag, steps)
        for copy in outputs(y):
            copy.start()
        return carry

    lax.fori_loop(0, rows, row_body, 0)
    for copy in early + [copy for y in range(rows) for copy in outputs(y)]:
        copy.wait()


def finish(control, state_buffer, packed, gradient, table, labels):
    steps, rows, planes, width = control.shape
    f32, dma = jnp.float32, pltpu.SemaphoreType.DMA
    in_vmem = pl.BlockSpec(memory_space=pltpu.VMEM)
    spectrum_shape = jax.ShapeDtypeStruct((2,) + control.shape, f32)
    return pl.pallas_call(
        finish_kernel,
        out_shape=(spectrum_shape, spectrum_shape, jax.ShapeDtypeStruct(control.shape, f32)),
        in_specs=[in_vmem] * 5,
        out_specs=(HBM,) * 3,
        scratch_shapes=[
            pltpu.VMEM((2, rows, steps, planes, width), f32),
            dma((2, rows)),
            dma((2, rows)),
            dma((rows,)),
        ],
        compiler_params=pltpu.CompilerParams(vmem_limit_bytes=16 * 2**20),
        name="finish",
    )(state_buffer, packed, gradient, table, labels)


def on_device(count, *arrays):
    state, adjoint, control, target, mask, regions = (
        pltpu.with_memory_space_constraint(array, pltpu.HBM) for array in arrays
    )
    found = solve(count, state, adjoint, control, regions, target, mask)
    return finish(control, *found)


def solution(mesh):
    return jax.shard_map(
        functools.partial(on_device, mesh.shape["space"]),
        mesh=mesh,
        in_specs=(
            P("parts", "space", None, None),
            P("parts", "space", None, None),
            P("parts", "space", None, None),
            P("parts", None),
            P("space", "parts"),
            P("space", "parts", None),
        ),
        out_specs=(
            P(None, "parts", "space", None, None),
            P(None, "parts", "space", None, None),
            P("parts", "space", None, None),
        ),
        check_vma=False,
    )
```

```python
import functools
import math

import jax
import jax.numpy as jnp
from jax import lax
from jax.experimental import pallas as pl
from jax.experimental.pallas import tpu as pltpu
from jax.sharding import PartitionSpec as P

time_step = 0.15
penalty = 0.5
MESH = pl.DeviceIdType.MESH
HBM = pl.BlockSpec(memory_space=pltpu.HBM)


def real_transform(values):
    n = len(values)
    if n == 1:
        return [values[0]], [None]
    if n % 2:
        real, imag = [], []
        for k in range(n // 2 + 1):
            angles = [2.0 * math.pi * (j * k % n) / n for j in range(n)]
            real.append(sum(v * math.cos(a) for v, a in zip(values, angles)))
            imag.append(None if k == 0 else sum(v * -math.sin(a) for v, a in zip(values, angles)))
        return real, imag
    even_re, even_im = real_transform(values[::2])
    odd_re, odd_im = real_transform(values[1::2])
    m = n // 2
    real, imag = [None] * (m + 1), [None] * (m + 1)
    for k in range(m // 2 + 1):
        a_re, a_im, b_re, b_im = even_re[k], even_im[k], odd_re[k], odd_im[k]
        if k == 0:
            real[0], real[m] = a_re + b_re, a_re - b_re
            continue
        if 2 * k == m:
            real[k], imag[k] = a_re, -b_re
            continue
        c, s = math.cos(2.0 * math.pi * k / n), math.sin(2.0 * math.pi * k / n)
        t_re, t_im = c * b_re + s * b_im, c * b_im - s * b_re
        real[k], imag[k] = a_re + t_re, a_im + t_im
        real[m - k], imag[m - k] = a_re - t_re, t_im - a_im
    return real, imag


def write_spectrum(buffer, row, lanes, real, imag, n):
    zero = jnp.zeros_like(real[0])
    for k in range(n):
        low = min(k, n - k)
        buffer[0, row, k, :, lanes] = real[low]
        value = imag[low]
        buffer[1, row, k, :, lanes] = zero if value is None else (value if k == low else -value)


def pack(real, imag):
    return real + [value for value in imag if value is not None]


def solve_kernel(
    count, state, adjoint, control, regions, target, mask,
    state_buffer, packed, gradient, table, labels,
    sampled, held, multipliers, heat, wanted, allowed, residual, partial, paired, joined, crossed, summed, gathered,
    small_sem, sample_sem, held_sem, mult_sem, heat_sem,
    halo_send, halo_recv, pair_send, pair_recv, chain_send, chain_recv,
):
    steps, rows, planes, width = control.shape
    count_regions = target.shape[1]
    blocks = width // 128
    links = count // 4
    me = lax.axis_index("space")
    link, place = me // 4, me % 4
    above, below = (me + 1) % count, (me + count - 1) % count
    partner = (me // 2) * 2 + 1 - me % 2
    across = link * 4 + (place + 2) % 4
    peers = [((link + d) % links) * 4 + place for d in range(1, links)]

    barrier = pltpu.get_barrier_semaphore()

    def greet(other):
        pl.semaphore_signal(barrier, inc=1, device_id={"space": other}, device_id_type=MESH)

    for other in [above, below, across] + peers:
        greet(other)

    sums_loads = [pltpu.make_async_copy(regions, labels, small_sem.at[0])] + [
        pltpu.make_async_copy(
            state.at[pl.ds(1, steps), :, :, pl.ds(block * 128, 128)],
            sampled.at[block], sample_sem.at[block],
        )
        for block in range(blocks)
    ]
    small_loads = [
        pltpu.make_async_copy(target, wanted, small_sem.at[1]),
        pltpu.make_async_copy(mask, allowed, small_sem.at[2]),
    ]
    heat_loads, mult_loads, held_loads = [], [], []
    for y in range(rows):
        heat_loads.append(pltpu.make_async_copy(control.at[pl.ds(0, steps), y], heat.at[y], heat_sem.at[y]))
        mult_loads.append(
            pltpu.make_async_copy(adjoint.at[pl.ds(0, steps), y], multipliers.at[y + 1], mult_sem.at[y])
        )
        held_loads.append(
            pltpu.make_async_copy(state.at[pl.ds(0, steps + 1), y], held.at[y + 1], held_sem.at[y])
        )
    for load in sums_loads + small_loads + heat_loads + mult_loads + held_loads:
        load.start()

    copies = []
    for source, first, target_rows, shift, length in (
        (state, 0, held, 0, steps), (adjoint, 1, multipliers, 1, steps - 1),
    ):
        for block in range(blocks):
            lanes = pl.ds(block * 128, 128)
            for row, into, other in ((rows - 1, 0, above), (0, rows + 1, below)):
                n = len(copies)
                copies.append(
                    pltpu.make_async_remote_copy(
                        src_ref=source.at[pl.ds(first, length), row, :, lanes],
                        dst_ref=target_rows.at[into, pl.ds(shift, length), :, lanes],
                        send_sem=halo_send.at[n],
                        recv_sem=halo_recv.at[n],
                        device_id={"space": other},
                        device_id_type=MESH,
                    )
                )

    flat = sampled.reshape(blocks, steps * rows * planes, 128)
    region_ids = lax.broadcasted_iota(jnp.int32, (count_regions, width), 0)

    def add_row(row, total):
        values = jnp.concatenate(
            [
                flat[block, pl.ds(row * planes + plane, steps, stride=rows * planes), :]
                for plane in range(planes)
                for block in range(blocks)
            ],
            axis=1,
        )
        high = values.astype(jnp.bfloat16)
        low = (values - high.astype(jnp.float32)).astype(jnp.bfloat16)
        ones = jnp.ones((16, planes * width), jnp.bfloat16)
        stacked = jnp.concatenate([high, low, ones], axis=0)
        onehot = jnp.concatenate(
            [
                (labels[row, pl.ds(plane, 1), :] == region_ids).astype(jnp.float32).astype(jnp.bfloat16)
                for plane in range(planes)
            ],
            axis=1,
        )
        return total + lax.dot_general(
            stacked, onehot, (((1,), (1,)), ((), ())), preferred_element_type=jnp.float32
        )

    pl.semaphore_wait(barrier, 3 + len(peers))
    for copy in copies[:2]:
        copy.start()
    for load in sums_loads:
        load.wait()
    total = jnp.zeros((2 * steps + 16, count_regions), jnp.float32)
    total = lax.fori_loop(0, rows, add_row, total)
    partial[:steps] = total[:steps] + total[steps : 2 * steps]
    partial[steps:] = total[2 * steps : 2 * steps + 8]
    pair = pltpu.make_async_remote_copy(
        src_ref=partial, dst_ref=paired, send_sem=pair_send.at[0], recv_sem=pair_recv.at[0],
        device_id={"space": partner}, device_id_type=MESH,
    )
    pair.start()

    lane = lax.broadcasted_iota(jnp.int32, (planes, width), 1)
    plane_ids = lax.broadcasted_iota(jnp.int32, (planes, width), 0)
    first_lane, last_lane = lane == 0, lane == width - 1
    first_plane, last_plane = plane_ids == 0, plane_ids == planes - 1

    def support_of(y):
        support = jnp.zeros((planes, width), jnp.float32)
        for plane in range(planes):
            support = jnp.where(plane_ids == plane, allowed[y, plane].astype(jnp.float32), support)
        return support

    for load in small_loads + heat_loads + mult_loads:
        load.wait()

    def gradient_row(y, carry):
        support = support_of(y)

        def step(j, inner):
            gradient[y, j] = penalty * heat[y, j] - support * multipliers[y + 1, j]
            return inner

        return lax.fori_loop(0, steps, step, carry, unroll=True)

    lax.fori_loop(0, rows, gradient_row, 0)

    pair.wait()
    joined[...] = partial[...] + paired[...]
    cross = pltpu.make_async_remote_copy(
        src_ref=joined, dst_ref=crossed, send_sem=pair_send.at[1], recv_sem=pair_recv.at[1],
        device_id={"space": across}, device_id_type=MESH,
    )
    cross.start()
    for copy in copies[2:4]:
        copy.start()

    sends = [
        pltpu.make_async_remote_copy(
            src_ref=summed, dst_ref=gathered.at[d], send_sem=chain_send.at[d], recv_sem=chain_recv.at[d],
            device_id={"space": peer}, device_id_type=MESH,
        )
        for d, peer in enumerate(peers)
    ]

    def laplace(values, beside):
        total = beside + jnp.where(first_lane, 0.0, pltpu.roll(values, 1, 1))
        total = total + jnp.where(last_lane, 0.0, pltpu.roll(values, width - 1, 1))
        total = total + jnp.where(first_plane, 0.0, pltpu.roll(values, 1, 0))
        total = total + jnp.where(last_plane, 0.0, pltpu.roll(values, planes - 1, 0))
        return total - 6.0 * values

    def adjoint_transform(y, beside):
        def step(j, carry):
            later = multipliers[y + 1, j + 1]
            residual[j] = multipliers[y + 1, j] - later - time_step * laplace(later, beside(j + 1))
            return carry

        lax.fori_loop(0, steps - 1, step, 0, unroll=True)
        residual[steps - 1] = multipliers[y + 1, steps - 1]
        for block in range(blocks):
            lanes = pl.ds(block * 128, 128)
            values = real_transform([residual[j, :, lanes] for j in range(steps)])
            for k, value in enumerate(pack(*values)):
                packed[y, k, :, lanes] = value

    def adjoint_inner(y, carry):
        adjoint_transform(y, lambda j: multipliers[y, j] + multipliers[y + 2, j])
        return carry

    def adjoint_edge(side, carry):
        adjoint_transform(side * (rows - 1), lambda j: multipliers[2 + side * (rows - 3), j])
        return carry

    def state_row(y, carry):
        support = support_of(y)

        def step(j, inner):
            now = held[y + 1, j]
            lap = laplace(now, held[y, j] + held[y + 2, j])
            residual[j] = held[y + 1, j + 1] - now - time_step * lap - time_step * support * heat[y, j]
            return inner

        lax.fori_loop(0, steps, step, 0, unroll=True)
        for block in range(blocks):
            lanes = pl.ds(block * 128, 128)
            real, imag = real_transform([residual[j, :, lanes] for j in range(steps)])
            write_spectrum(state_buffer, y, lanes, real, imag, steps)
        return carry

    lax.fori_loop(1, rows - 1, adjoint_inner, 0)
    cross.wait()
    summed[...] = joined[...] + crossed[...]
    for send in sends:
        send.start()
    for copy in copies[4:]:
        copy.start()
    lax.fori_loop(0, 2, adjoint_edge, 0)
    for load in held_loads:
        load.wait()
    lax.fori_loop(1, rows - 1, state_row, 0)
    for copy in copies[: 2 * blocks]:
        copy.wait()
    lax.fori_loop(0, 2, lambda side, carry: state_row(side * (rows - 1), carry), 0)

    result = summed[...]
    for d, send in enumerate(sends):
        send.wait()
        result = result + gathered[d]
    misfit = result[:steps] / result[steps : steps + 1] - wanted[...]
    values = real_transform(
        [jnp.broadcast_to(misfit[j : j + 1], (8, count_regions)) for j in range(steps)]
    )
    for k, value in enumerate(pack(*values)):
        table[k] = value

    for block in range(blocks):
        lanes = pl.ds(block * 128, 128)
        for side in range(2):
            copies[2 * (blocks + block) + side].wait()

        def add_halo(side, carry):
            y, outer = side * (rows - 1), side * (rows + 1)
            values = [-time_step * multipliers[outer, j + 1, :, lanes] for j in range(steps - 1)]
            values.append(jnp.zeros_like(values[0]))
            for k, value in enumerate(pack(*real_transform(values))):
                packed[y, k, :, lanes] += value
            return carry

        lax.fori_loop(0, 2, add_halo, 0)


def solve(count, state, adjoint, control, regions, target, mask):
    steps, rows, planes, width = control.shape
    count_regions = target.shape[1]
    padded = (steps + 8, count_regions)
    blocks = width // 128
    f32, dma, vmem = jnp.float32, pltpu.SemaphoreType.DMA, pltpu.VMEM
    in_vmem = pl.BlockSpec(memory_space=pltpu.VMEM)
    return pl.pallas_call(
        functools.partial(solve_kernel, count),
        out_shape=(
            vmem((2, rows, steps, planes, width), f32),
            vmem((rows, steps, planes, width), f32),
            vmem((rows, steps, planes, width), f32),
            vmem((steps, 8, count_regions), f32),
            vmem(regions.shape, jnp.int32),
        ),
        in_specs=[HBM] * 6,
        out_specs=(in_vmem,) * 5,
        scratch_shapes=[
            vmem((blocks, steps, rows, planes, 128), f32),
            vmem((rows + 2, steps + 1, planes, width), f32),
            vmem((rows + 2, steps, planes, width), f32),
            vmem((rows, steps, planes, width), f32),
            vmem(target.shape, f32),
            pltpu.SMEM(mask.shape, jnp.int32),
            vmem((steps, planes, width), f32),
        ]
        + [vmem(padded, f32)] * 5
        + [
            vmem((count // 4 - 1,) + padded, f32),
            dma((3,)),
            dma((blocks,)),
            dma((rows,)),
            dma((rows,)),
            dma((rows,)),
            dma((4 * blocks,)),
            dma((4 * blocks,)),
            dma((2,)),
            dma((2,)),
            dma((count // 4 - 1,)),
            dma((count // 4 - 1,)),
        ],
        compiler_params=pltpu.CompilerParams(
            collective_id=0, has_side_effects=True, vmem_limit_bytes=24 * 2**20
        ),
        name="solve",
    )(state, adjoint, control, regions, target, mask)


def finish_kernel(
    state_buffer, packed, gradient, table, labels,
    state_out, adjoint_out, gradient_out,
    adjoint_buffer, state_sem, adjoint_sem, gradient_sem,
):
    rows, steps, planes, width = gradient.shape
    early = []
    for y in range(rows):
        for part in range(2):
            early.append(
                pltpu.make_async_copy(
                    state_buffer.at[part, y], state_out.at[part, pl.ds(0, steps), y], state_sem.at[part, y]
                )
            )
        early.append(
            pltpu.make_async_copy(gradient.at[y], gradient_out.at[pl.ds(0, steps), y], gradient_sem.at[y])
        )
    for copy in early:
        copy.start()

    def outputs(y):
        return [
            pltpu.make_async_copy(
                adjoint_buffer.at[part, y], adjoint_out.at[part, pl.ds(0, steps), y], adjoint_sem.at[part, y]
            )
            for part in range(2)
        ]

    def row_body(y, carry):
        for block in range(width // 128):
            lanes = pl.ds(block * 128, 128)
            ids = labels[y, :, lanes]
            values = [
                packed[y, k, :, lanes] + jnp.take_along_axis(table[k], ids, axis=1, mode="promise_in_bounds")
                for k in range(steps)
            ]
            top = steps // 2 + 1
            imag = [None] + values[top:] + [None] * (2 * top - 1 - steps)
            write_spectrum(adjoint_buffer, y, lanes, values[:top], imag, steps)
        for copy in outputs(y):
            copy.start()
        return carry

    lax.fori_loop(0, rows, row_body, 0)
    for copy in early + [copy for y in range(rows) for copy in outputs(y)]:
        copy.wait()


def finish(control, state_buffer, packed, gradient, table, labels):
    steps, rows, planes, width = control.shape
    f32, dma = jnp.float32, pltpu.SemaphoreType.DMA
    in_vmem = pl.BlockSpec(memory_space=pltpu.VMEM)
    spectrum_shape = jax.ShapeDtypeStruct((2,) + control.shape, f32)
    return pl.pallas_call(
        finish_kernel,
        out_shape=(spectrum_shape, spectrum_shape, jax.ShapeDtypeStruct(control.shape, f32)),
        in_specs=[in_vmem] * 5,
        out_specs=(HBM,) * 3,
        scratch_shapes=[
            pltpu.VMEM((2, rows, steps, planes, width), f32),
            dma((2, rows)),
            dma((2, rows)),
            dma((rows,)),
        ],
        compiler_params=pltpu.CompilerParams(vmem_limit_bytes=16 * 2**20),
        name="finish",
    )(state_buffer, packed, gradient, table, labels)


def on_device(count, *arrays):
    state, adjoint, control, target, mask, regions = (
        pltpu.with_memory_space_constraint(array, pltpu.HBM) for array in arrays
    )
    found = solve(count, state, adjoint, control, regions, target, mask)
    return finish(control, *found)


def solution(mesh):
    return jax.shard_map(
        functools.partial(on_device, mesh.shape["space"]),
        mesh=mesh,
        in_specs=(
            P("parts", "space", None, None),
            P("parts", "space", None, None),
            P("parts", "space", None, None),
            P("parts", None),
            P("space", "parts"),
            P("space", "parts", None),
        ),
        out_specs=(
            P(None, "parts", "space", None, None),
            P(None, "parts", "space", None, None),
            P("parts", "space", None, None),
        ),
        check_vma=False,
    )
```

```python
import functools
import math

import jax
import jax.numpy as jnp
from jax import lax
from jax.experimental import pallas as pl
from jax.experimental.pallas import tpu as pltpu
from jax.sharding import PartitionSpec as P

time_step = 0.15
penalty = 0.5
MESH = pl.DeviceIdType.MESH
HBM = pl.BlockSpec(memory_space=pltpu.HBM)


def real_transform(values):
    n = len(values)
    if n == 1:
        return [values[0]], [None]
    if n % 2:
        real, imag = [], []
        for k in range(n // 2 + 1):
            angles = [2.0 * math.pi * (j * k % n) / n for j in range(n)]
            real.append(sum(v * math.cos(a) for v, a in zip(values, angles)))
            imag.append(None if k == 0 else sum(v * -math.sin(a) for v, a in zip(values, angles)))
        return real, imag
    even_re, even_im = real_transform(values[::2])
    odd_re, odd_im = real_transform(values[1::2])
    m = n // 2
    real, imag = [None] * (m + 1), [None] * (m + 1)
    for k in range(m // 2 + 1):
        a_re, a_im, b_re, b_im = even_re[k], even_im[k], odd_re[k], odd_im[k]
        if k == 0:
            real[0], real[m] = a_re + b_re, a_re - b_re
            continue
        if 2 * k == m:
            real[k], imag[k] = a_re, -b_re
            continue
        c, s = math.cos(2.0 * math.pi * k / n), math.sin(2.0 * math.pi * k / n)
        t_re, t_im = c * b_re + s * b_im, c * b_im - s * b_re
        real[k], imag[k] = a_re + t_re, a_im + t_im
        real[m - k], imag[m - k] = a_re - t_re, t_im - a_im
    return real, imag


def write_spectrum(buffer, row, lanes, real, imag, n):
    zero = jnp.zeros_like(real[0])
    for k in range(n):
        low = min(k, n - k)
        buffer[0, row, k, :, lanes] = real[low]
        value = imag[low]
        buffer[1, row, k, :, lanes] = zero if value is None else (value if k == low else -value)


def pack(real, imag):
    return real + [value for value in imag if value is not None]


def solve_kernel(
    count, state, adjoint, control, regions, target, mask,
    state_buffer, packed, gradient, table, labels,
    sampled, held, multipliers, heat, wanted, allowed, residual, partial, paired, joined, crossed, summed, gathered,
    small_sem, sample_sem, held_sem, mult_sem, heat_sem,
    halo_send, halo_recv, pair_send, pair_recv, chain_send, chain_recv, known,
):
    steps, rows, planes, width = control.shape
    count_regions = target.shape[1]
    blocks = width // 128
    links = count // 4
    me = lax.axis_index("space")
    link, place = me // 4, me % 4
    above, below = (me + 1) % count, (me + count - 1) % count
    partner = (me // 2) * 2 + 1 - me % 2
    across = link * 4 + (place + 2) % 4
    peers = [((link + d) % links) * 4 + place for d in range(1, links)]

    barrier = pltpu.get_barrier_semaphore()

    def greet(other):
        pl.semaphore_signal(barrier, inc=1, device_id={"space": other}, device_id_type=MESH)

    upper, lower = (me + 4) % count, (me + count - 4) % count
    has_upper, has_lower = link < links - 1, link > 0
    beside_count = has_upper.astype(jnp.int32) + has_lower.astype(jnp.int32)
    for other in (above, below, across):
        greet(other)
    pl.when(has_upper)(lambda: greet(upper))
    pl.when(has_lower)(lambda: greet(lower))

    def tell(turn):
        def to(other):
            pl.semaphore_signal(
                known.at[turn], inc=1, device_id={"space": other}, device_id_type=MESH
            )

        pl.when(has_upper)(lambda: to(upper))
        pl.when(has_lower)(lambda: to(lower))

    turns = links - 2

    sums_loads = [pltpu.make_async_copy(regions, labels, small_sem.at[0])] + [
        pltpu.make_async_copy(
            state.at[pl.ds(1, steps), :, :, pl.ds(block * 128, 128)],
            sampled.at[block], sample_sem.at[block],
        )
        for block in range(blocks)
    ]
    small_loads = [
        pltpu.make_async_copy(target, wanted, small_sem.at[1]),
        pltpu.make_async_copy(mask, allowed, small_sem.at[2]),
    ]
    heat_loads, mult_loads, held_loads = [], [], []
    for y in range(rows):
        heat_loads.append(pltpu.make_async_copy(control.at[pl.ds(0, steps), y], heat.at[y], heat_sem.at[y]))
        mult_loads.append(
            pltpu.make_async_copy(adjoint.at[pl.ds(0, steps), y], multipliers.at[y + 1], mult_sem.at[y])
        )
        held_loads.append(
            pltpu.make_async_copy(state.at[pl.ds(0, steps + 1), y], held.at[y + 1], held_sem.at[y])
        )
    for load in sums_loads + small_loads + heat_loads + mult_loads + held_loads:
        load.start()

    copies = []
    for source, first, target_rows, shift, length in (
        (state, 0, held, 0, steps), (adjoint, 1, multipliers, 1, steps - 1),
    ):
        for block in range(blocks):
            lanes = pl.ds(block * 128, 128)
            for row, into, other in ((rows - 1, 0, above), (0, rows + 1, below)):
                n = len(copies)
                copies.append(
                    pltpu.make_async_remote_copy(
                        src_ref=source.at[pl.ds(first, length), row, :, lanes],
                        dst_ref=target_rows.at[into, pl.ds(shift, length), :, lanes],
                        send_sem=halo_send.at[n],
                        recv_sem=halo_recv.at[n],
                        device_id={"space": other},
                        device_id_type=MESH,
                    )
                )

    flat = sampled.reshape(blocks, steps * rows * planes, 128)
    region_ids = lax.broadcasted_iota(jnp.int32, (count_regions, width), 0)

    def add_row(row, total):
        values = jnp.concatenate(
            [
                flat[block, pl.ds(row * planes + plane, steps, stride=rows * planes), :]
                for plane in range(planes)
                for block in range(blocks)
            ],
            axis=1,
        )
        high = values.astype(jnp.bfloat16)
        low = (values - high.astype(jnp.float32)).astype(jnp.bfloat16)
        ones = jnp.ones((16, planes * width), jnp.bfloat16)
        stacked = jnp.concatenate([high, low, ones], axis=0)
        onehot = jnp.concatenate(
            [
                (labels[row, pl.ds(plane, 1), :] == region_ids).astype(jnp.float32).astype(jnp.bfloat16)
                for plane in range(planes)
            ],
            axis=1,
        )
        return total + lax.dot_general(
            stacked, onehot, (((1,), (1,)), ((), ())), preferred_element_type=jnp.float32
        )

    pl.semaphore_wait(barrier, 3 + beside_count)
    if turns > 0:
        tell(0)
    for copy in copies[:2]:
        copy.start()
    for load in sums_loads:
        load.wait()
    total = jnp.zeros((2 * steps + 16, count_regions), jnp.float32)
    total = lax.fori_loop(0, rows, add_row, total)
    partial[:steps] = total[:steps] + total[steps : 2 * steps]
    partial[steps:] = total[2 * steps : 2 * steps + 8]
    pair = pltpu.make_async_remote_copy(
        src_ref=partial, dst_ref=paired, send_sem=pair_send.at[0], recv_sem=pair_recv.at[0],
        device_id={"space": partner}, device_id_type=MESH,
    )
    pair.start()

    lane = lax.broadcasted_iota(jnp.int32, (planes, width), 1)
    plane_ids = lax.broadcasted_iota(jnp.int32, (planes, width), 0)
    first_lane, last_lane = lane == 0, lane == width - 1
    first_plane, last_plane = plane_ids == 0, plane_ids == planes - 1

    def support_of(y):
        support = jnp.zeros((planes, width), jnp.float32)
        for plane in range(planes):
            support = jnp.where(plane_ids == plane, allowed[y, plane].astype(jnp.float32), support)
        return support

    for load in small_loads + heat_loads + mult_loads:
        load.wait()

    def gradient_row(y, carry):
        support = support_of(y)

        def step(j, inner):
            gradient[y, j] = penalty * heat[y, j] - support * multipliers[y + 1, j]
            return inner

        return lax.fori_loop(0, steps, step, carry, unroll=True)

    lax.fori_loop(0, rows, gradient_row, 0)

    pair.wait()
    joined[...] = partial[...] + paired[...]
    cross = pltpu.make_async_remote_copy(
        src_ref=joined, dst_ref=crossed, send_sem=pair_send.at[1], recv_sem=pair_recv.at[1],
        device_id={"space": across}, device_id_type=MESH,
    )
    cross.start()
    for copy in copies[2:4]:
        copy.start()

    sends = [
        pltpu.make_async_remote_copy(
            src_ref=summed, dst_ref=gathered.at[d], send_sem=chain_send.at[d], recv_sem=chain_recv.at[d],
            device_id={"space": peer}, device_id_type=MESH,
        )
        for d, peer in enumerate(peers)
    ]

    def laplace(values, beside):
        total = beside + jnp.where(first_lane, 0.0, pltpu.roll(values, 1, 1))
        total = total + jnp.where(last_lane, 0.0, pltpu.roll(values, width - 1, 1))
        total = total + jnp.where(first_plane, 0.0, pltpu.roll(values, 1, 0))
        total = total + jnp.where(last_plane, 0.0, pltpu.roll(values, planes - 1, 0))
        return total - 6.0 * values

    def adjoint_transform(y, beside):
        def step(j, carry):
            later = multipliers[y + 1, j + 1]
            residual[j] = multipliers[y + 1, j] - later - time_step * laplace(later, beside(j + 1))
            return carry

        lax.fori_loop(0, steps - 1, step, 0, unroll=True)
        residual[steps - 1] = multipliers[y + 1, steps - 1]
        for block in range(blocks):
            lanes = pl.ds(block * 128, 128)
            values = real_transform([residual[j, :, lanes] for j in range(steps)])
            for k, value in enumerate(pack(*values)):
                packed[y, k, :, lanes] = value

    def adjoint_inner(y, carry):
        adjoint_transform(y, lambda j: multipliers[y, j] + multipliers[y + 2, j])
        return carry

    def adjoint_edge(side, carry):
        adjoint_transform(side * (rows - 1), lambda j: multipliers[2 + side * (rows - 3), j])
        return carry

    def state_row(y, carry):
        support = support_of(y)

        def step(j, inner):
            now = held[y + 1, j]
            lap = laplace(now, held[y, j] + held[y + 2, j])
            residual[j] = held[y + 1, j + 1] - now - time_step * lap - time_step * support * heat[y, j]
            return inner

        lax.fori_loop(0, steps, step, 0, unroll=True)
        for block in range(blocks):
            lanes = pl.ds(block * 128, 128)
            real, imag = real_transform([residual[j, :, lanes] for j in range(steps)])
            write_spectrum(state_buffer, y, lanes, real, imag, steps)
        return carry

    lax.fori_loop(1, rows - 1, adjoint_inner, 0)
    cross.wait()
    summed[...] = joined[...] + crossed[...]
    for turn in range(max(turns, 0)):
        pl.semaphore_wait(known.at[turn], beside_count)
        if turn + 1 < turns:
            tell(turn + 1)
    for send in sends:
        send.start()
    for copy in copies[4:]:
        copy.start()
    lax.fori_loop(0, 2, adjoint_edge, 0)
    for load in held_loads:
        load.wait()
    lax.fori_loop(1, rows - 1, state_row, 0)
    for copy in copies[: 2 * blocks]:
        copy.wait()
    lax.fori_loop(0, 2, lambda side, carry: state_row(side * (rows - 1), carry), 0)

    result = summed[...]
    for d, send in enumerate(sends):
        send.wait()
        result = result + gathered[d]
    misfit = result[:steps] / result[steps : steps + 1] - wanted[...]
    values = real_transform(
        [jnp.broadcast_to(misfit[j : j + 1], (8, count_regions)) for j in range(steps)]
    )
    for k, value in enumerate(pack(*values)):
        table[k] = value

    for block in range(blocks):
        lanes = pl.ds(block * 128, 128)
        for side in range(2):
            copies[2 * (blocks + block) + side].wait()

        def add_halo(side, carry):
            y, outer = side * (rows - 1), side * (rows + 1)
            values = [-time_step * multipliers[outer, j + 1, :, lanes] for j in range(steps - 1)]
            values.append(jnp.zeros_like(values[0]))
            for k, value in enumerate(pack(*real_transform(values))):
                packed[y, k, :, lanes] += value
            return carry

        lax.fori_loop(0, 2, add_halo, 0)


def solve(count, state, adjoint, control, regions, target, mask):
    steps, rows, planes, width = control.shape
    count_regions = target.shape[1]
    padded = (steps + 8, count_regions)
    blocks = width // 128
    f32, dma, vmem = jnp.float32, pltpu.SemaphoreType.DMA, pltpu.VMEM
    in_vmem = pl.BlockSpec(memory_space=pltpu.VMEM)
    return pl.pallas_call(
        functools.partial(solve_kernel, count),
        out_shape=(
            vmem((2, rows, steps, planes, width), f32),
            vmem((rows, steps, planes, width), f32),
            vmem((rows, steps, planes, width), f32),
            vmem((steps, 8, count_regions), f32),
            vmem(regions.shape, jnp.int32),
        ),
        in_specs=[HBM] * 6,
        out_specs=(in_vmem,) * 5,
        scratch_shapes=[
            vmem((blocks, steps, rows, planes, 128), f32),
            vmem((rows + 2, steps + 1, planes, width), f32),
            vmem((rows + 2, steps, planes, width), f32),
            vmem((rows, steps, planes, width), f32),
            vmem(target.shape, f32),
            pltpu.SMEM(mask.shape, jnp.int32),
            vmem((steps, planes, width), f32),
        ]
        + [vmem(padded, f32)] * 5
        + [
            vmem((count // 4 - 1,) + padded, f32),
            dma((3,)),
            dma((blocks,)),
            dma((rows,)),
            dma((rows,)),
            dma((rows,)),
            dma((4 * blocks,)),
            dma((4 * blocks,)),
            dma((2,)),
            dma((2,)),
            dma((count // 4 - 1,)),
            dma((count // 4 - 1,)),
            pltpu.SemaphoreType.REGULAR((max(count // 4 - 2, 1),)),
        ],
        compiler_params=pltpu.CompilerParams(
            collective_id=0, has_side_effects=True, vmem_limit_bytes=24 * 2**20
        ),
        name="solve",
    )(state, adjoint, control, regions, target, mask)


def finish_kernel(
    state_buffer, packed, gradient, table, labels,
    state_out, adjoint_out, gradient_out,
    adjoint_buffer, state_sem, adjoint_sem, gradient_sem,
):
    rows, steps, planes, width = gradient.shape
    early = []
    for y in range(rows):
        for part in range(2):
            early.append(
                pltpu.make_async_copy(
                    state_buffer.at[part, y], state_out.at[part, pl.ds(0, steps), y], state_sem.at[part, y]
                )
            )
        early.append(
            pltpu.make_async_copy(gradient.at[y], gradient_out.at[pl.ds(0, steps), y], gradient_sem.at[y])
        )
    for copy in early:
        copy.start()

    def outputs(y):
        return [
            pltpu.make_async_copy(
                adjoint_buffer.at[part, y], adjoint_out.at[part, pl.ds(0, steps), y], adjoint_sem.at[part, y]
            )
            for part in range(2)
        ]

    def row_body(y, carry):
        for block in range(width // 128):
            lanes = pl.ds(block * 128, 128)
            ids = labels[y, :, lanes]
            values = [
                packed[y, k, :, lanes] + jnp.take_along_axis(table[k], ids, axis=1, mode="promise_in_bounds")
                for k in range(steps)
            ]
            top = steps // 2 + 1
            imag = [None] + values[top:] + [None] * (2 * top - 1 - steps)
            write_spectrum(adjoint_buffer, y, lanes, values[:top], imag, steps)
        for copy in outputs(y):
            copy.start()
        return carry

    lax.fori_loop(0, rows, row_body, 0)
    for copy in early + [copy for y in range(rows) for copy in outputs(y)]:
        copy.wait()


def finish(control, state_buffer, packed, gradient, table, labels):
    steps, rows, planes, width = control.shape
    f32, dma = jnp.float32, pltpu.SemaphoreType.DMA
    in_vmem = pl.BlockSpec(memory_space=pltpu.VMEM)
    spectrum_shape = jax.ShapeDtypeStruct((2,) + control.shape, f32)
    return pl.pallas_call(
        finish_kernel,
        out_shape=(spectrum_shape, spectrum_shape, jax.ShapeDtypeStruct(control.shape, f32)),
        in_specs=[in_vmem] * 5,
        out_specs=(HBM,) * 3,
        scratch_shapes=[
            pltpu.VMEM((2, rows, steps, planes, width), f32),
            dma((2, rows)),
            dma((2, rows)),
            dma((rows,)),
        ],
        compiler_params=pltpu.CompilerParams(vmem_limit_bytes=16 * 2**20),
        name="finish",
    )(state_buffer, packed, gradient, table, labels)


def on_device(count, *arrays):
    state, adjoint, control, target, mask, regions = (
        pltpu.with_memory_space_constraint(array, pltpu.HBM) for array in arrays
    )
    found = solve(count, state, adjoint, control, regions, target, mask)
    return finish(control, *found)


def solution(mesh):
    return jax.shard_map(
        functools.partial(on_device, mesh.shape["space"]),
        mesh=mesh,
        in_specs=(
            P("parts", "space", None, None),
            P("parts", "space", None, None),
            P("parts", "space", None, None),
            P("parts", None),
            P("space", "parts"),
            P("space", "parts", None),
        ),
        out_specs=(
            P(None, "parts", "space", None, None),
            P(None, "parts", "space", None, None),
            P("parts", "space", None, None),
        ),
        check_vma=False,
    )
```
